256 devices in a mesh: dp: 32 (over z, x_hi, core), expert: 8 (over x_lo, y).
Axes of the slice: x: 4 (x_hi: 2, x_lo: 2; x = x_hi * 2 + x_lo), y: 4, z: 8, core: 2. Of those that a mesh axis runs over, the one named last changes fastest.
Arguments:
- x_rows: bfloat16 [131072, 1024], P(('dp', 'expert')), may hold values from -24 to 24
- dy_rows: bfloat16 [131072, 2048], P(('dp', 'expert')), may hold values from -0.0234375 to 0.0234375
- seg_blocks: int32 [256, 8], replicated, may hold values from 0 to 2, as said below
Outputs:
- expert_grad: float32 [8, 1024, 2048], P(None, 'dp', 'expert')
The draws below stay inside these ranges and needn't reach their ends.
Inputs may be any that keep to these rules, and one draw needn't show every extreme that they name: `seg_blocks`: on every device the entries sum to at most 4; one expert has exactly 2 blocks on every device.
All inputs are finite; a program needn't handle non-finite values.
Results may differ from the reference program's by a relative error of at most 0.0003.
Values may be sent and summed in bfloat16 or wider, within the bound.
A program may use at most 128 MiB of HBM per device.

```python
import jax
import jax.numpy as jnp
from jax import lax

H = 1024
F = 2048
BLOCK = 128
CAP = 2
BLOCKS_DEV = 4
EXPERTS = 8
SHARDS = 256
ROWS = 131072


def draw_seg_blocks(key, part):
    hot = jax.random.randint(jax.random.fold_in(key, 7), (), 0, EXPERTS)
    room = min(BLOCKS_DEV, CAP * EXPERTS) - CAP
    experts_row = jnp.arange(EXPERTS, dtype=jnp.int32)

    def single(device):
        sub = jax.random.fold_in(jax.random.fold_in(key, 11), device)
        order = jax.random.permutation(sub, CAP * EXPERTS)
        slot_expert = (order // CAP).astype(jnp.int32)
        others = (slot_expert != hot).astype(jnp.int32)
        rank = jnp.cumsum(others) - 1
        taken = jax.random.randint(jax.random.fold_in(sub, 3), (), room // 2, room + 1)
        chosen = others * (rank < taken).astype(jnp.int32)
        counts = jnp.sum(chosen[:, None] * (slot_expert[:, None] == experts_row[None, :]).astype(jnp.int32), axis=0)
        return (counts + CAP * (experts_row == hot).astype(jnp.int32)).astype(jnp.int32)
    return jax.vmap(single)(jnp.arange(SHARDS, dtype=jnp.int32))


def strengthened(values, own_key, source, target, shards_of, factor):
    owner, partner = [(jnp.arange(values.shape[dim]) // (values.shape[dim] // shards_of)).reshape([-1 if axis == dim else 1 for axis in range(values.ndim)]) for dim in (source, target)]
    chosen = jax.random.permutation(own_key, shards_of)[partner]
    strong = (owner == chosen) | (owner == (partner + shards_of // 2) % shards_of)
    return jnp.where(strong, factor * values, values)


def steps_of(key, extent, shards, least, largest):
    level, own = 1.0, jax.random.fold_in(key, 6)
    for position, blocks in shards:
        draws = jnp.exp(jax.random.uniform(jax.random.fold_in(own, position), (blocks,), jnp.float32, least / len(shards), largest / len(shards)))
        level = level * jnp.repeat(draws, extent[position] // blocks).reshape([-1 if axis == position else 1 for axis in range(len(extent))])
    return level


def scatter_about(own_key, shape, width, limit, cuts=(), kind=jnp.bfloat16):
    values = width * jax.random.normal(own_key, shape, jnp.float32)
    if cuts:
        values = values * steps_of(own_key, shape, cuts, -0.22, 0.18)
    return jnp.clip(values, -limit, limit).astype(kind)


def gaussian_with(own_key, extent, deviation, bound, cuts, heavy, kind=jnp.bfloat16):
    array = deviation * jax.random.normal(own_key, extent, jnp.float32)
    if cuts:
        array = array * steps_of(own_key, extent, cuts, -0.22, 0.18)
    return jnp.clip(strengthened(array, jax.random.fold_in(own_key, 3), *heavy), -bound, bound).astype(kind)


def setup_inputs(seed: int = 0) -> dict:
    keys = jax.random.split(jax.random.key(seed), 4)
    return {
        "x_rows": gaussian_with(keys[0], (ROWS, H), 1.0, 24.0, ((0, 256),), (0, 1, 256, 6.0)),
        "dy_rows": scatter_about(keys[1], (ROWS, F), (SHARDS * CAP * BLOCK) ** -0.5, 0.0234375, ((0, 256),)),
        "seg_blocks": draw_seg_blocks(jax.random.fold_in(keys[3], 71), 0),
    }


def pack(xdev, dydev, counts):
    nblk = xdev.shape[0] // BLOCK
    counts = counts.astype(jnp.int32)
    starts = (jnp.cumsum(counts) - counts).astype(jnp.int32)
    slots = jnp.arange(CAP, dtype=jnp.int32)
    live = slots[None, :] < counts[:, None]
    index = jnp.where(live, starts[:, None] + slots[None, :], 0).reshape(-1).astype(jnp.int32)
    keep = live.reshape(-1)[:, None, None]
    xblk = jnp.where(keep, xdev.reshape(nblk, BLOCK, -1)[index], jnp.zeros((), xdev.dtype))
    dyblk = jnp.where(keep, dydev.reshape(nblk, BLOCK, -1)[index], jnp.zeros((), dydev.dtype))
    return xblk, dyblk


def reference(x_rows, dy_rows, seg_blocks):
    xs = x_rows.reshape(SHARDS, -1, H)
    dys = dy_rows.reshape(SHARDS, -1, F)

    def step(total, item):
        xdev, dydev, counts = item
        xblk, dyblk = pack(xdev, dydev, counts)
        xblk = xblk.reshape(EXPERTS, CAP * BLOCK, H).astype(jnp.float32)
        dyblk = dyblk.reshape(EXPERTS, CAP * BLOCK, F).astype(jnp.float32)
        return total + jnp.einsum("erh,erf->ehf", xblk, dyblk), None

    init = jnp.zeros((EXPERTS, H, F), jnp.float32)
    total, _ = lax.scan(step, init, (xs, dys, seg_blocks))
    return total
```

```python
import jax
import jax.numpy as jnp
from jax import lax
from jax.sharding import PartitionSpec as P

BLOCK = 128


def row_owners(seg_blocks, devices, nblk):
    counts = seg_blocks[devices]
    ends = jnp.cumsum(counts, axis=1)
    block = jnp.arange(nblk, dtype=jnp.int32)
    return jnp.sum((ends[:, None, :] <= block[None, :, None]).astype(jnp.int32), axis=2)


def shards(x_rows, dy_rows, seg_blocks):
    rows, hid = x_rows.shape
    ffn = dy_rows.shape[1]
    n_exp = lax.axis_size("expert")
    experts = seg_blocks.shape[1]
    nblk = rows // BLOCK
    devices = lax.axis_index("dp") * n_exp + jnp.arange(n_exp)
    owner = row_owners(seg_blocks, devices, nblk).reshape(-1)
    mask = (owner[None, :] == jnp.arange(experts)[:, None]).astype(x_rows.dtype)
    mask = jnp.repeat(mask, BLOCK, axis=1)
    xg = lax.all_gather(x_rows, "expert", axis=0, tiled=True)
    dyg = lax.all_to_all(dy_rows, "expert", split_axis=1, concat_axis=0, tiled=True)
    xm = (xg[None] * mask[:, :, None])
    part = jnp.einsum("eth,tf->ehf", xm, dyg, preferred_element_type=jnp.float32)
    return lax.psum_scatter(part, "dp", scatter_dimension=1, tiled=True)


def solution(mesh):
    in_specs = (P(("dp", "expert"), None), P(("dp", "expert"), None), P())
    out_specs = P(None, "dp", "expert")
    return jax.shard_map(shards, mesh=mesh, in_specs=in_specs, out_specs=out_specs, check_vma=False)
```

```python
import functools

import jax
import jax.numpy as jnp
from jax import lax
from jax.experimental import pallas as pl
from jax.experimental.pallas import tpu as pltpu
from jax.sharding import PartitionSpec as P

BLOCK = 128
NE = 8
NY, NX, NZ = 4, 4, 8
NG = 2 * NY
HR, FC = 32, 256
HALF = NE // 2
MSG = HALF * HR + 16
OFFS = (4, 3, -3, 2, -2, 1, -1, 0)
QMAX = 32700.0


def encode(dst, scales, get):
    for e in range(HALF):
        v = get(e)
        top = jnp.max(jnp.abs(v), axis=0, keepdims=True)
        lev = jnp.ceil(jnp.log2(jnp.maximum(top, 1e-30)) * 256.0) + 1.0
        q = jnp.round(v * (jnp.exp2(lev * (-1.0 / 256.0)) * QMAX))
        dst[e * HR:(e + 1) * HR, :] = q.astype(jnp.int32).astype(jnp.int16)
        scales[e:e + 1, :] = lev
    dst[HALF * HR:, :] = scales[...].astype(jnp.int32).astype(jnp.int16)


def decoder(src):
    lev = src[HALF * HR:, :].astype(jnp.int32).astype(jnp.float32)
    s = jnp.exp2(lev * (1.0 / 256.0)) * (1.0 / QMAX)

    def get(e):
        q = src[e * HR:(e + 1) * HR, :].astype(jnp.int32).astype(jnp.float32)
        return q * s[e:e + 1, :]
    return get


def kernel(xt, dy, msk, out, xg, dyg, rel, part, xa_s, xa_r, xb_s, xb_r, z_s, z_r, scales,
           dsem, xsem, asem, bsem, zsem):
    dp, ex = lax.axis_index("dp"), lax.axis_index("expert")
    z, xh, c = dp // 4, (dp // 2) % 2, dp % 2
    xl, y = ex // NY, ex % NY
    X = xh * 2 + xl

    def at(z_=z, x_=X, c_=c, y_=y):
        return (z_ * 4 + (x_ // 2) * 2 + c_, (x_ % 2) * NY + y_)

    yp, ym = (y + 1) % NY, (y + 3) % NY
    xp, xm = (X + 1) % NX, (X + 3) % NX
    zp, zm = (z + 1) % NZ, (z + 7) % NZ
    partner = at(c_=1 - c)
    up, down = at(y_=yp), at(y_=ym)
    right, left = at(x_=xp), at(x_=xm)
    ahead, behind = at(z_=zp), at(z_=zm)
    g_me, g_pa = y * 2 + c, y * 2 + 1 - c

    barrier = pltpu.get_barrier_semaphore()
    for other in (partner, up, down, right, left, ahead, behind):
        pl.semaphore_signal(barrier, inc=1, device_id=other, device_id_type=pl.DeviceIdType.MESH)
    scales[...] = jnp.zeros_like(scales)
    pl.semaphore_wait(barrier, 7)

    started = []

    def copy(src, dst, sem, dev):
        return pltpu.make_async_remote_copy(
            src_ref=src, dst_ref=dst, send_sem=sem.at[0], recv_sem=sem.at[1],
            device_id=dev, device_id_type=pl.DeviceIdType.MESH)

    def send(src, dst, sem, dev):
        op = copy(src, dst, sem, dev)
        op.start()
        started.append(op)

    def arrived(dst, sem):
        copy(dst, dst, sem, partner).wait_recv()

    def cols(yy, j):
        return dy.at[:, pl.ds(pl.multiple_of((j * NY + yy) * FC, FC), FC)]

    y2 = (y + 2) % NY
    send(cols(y2, 0), rel.at[0], dsem.at[0], up)
    send(cols(y2, 1), rel.at[1], dsem.at[1], down)
    send(xt.at[1 - c], xg.at[g_me], xsem.at[48], partner)
    for j in range(2):
        send(cols(yp, j), dyg.at[g_me, j], dsem.at[2 + j], up)
        send(cols(ym, j), dyg.at[g_me, j], dsem.at[4 + j], down)
        send(cols(y, j), dyg.at[g_me, j], dsem.at[6 + j], partner)
    for j in range(2):
        dyg[g_me, j] = dy[:, pl.ds(pl.multiple_of((j * NY + y) * FC, FC), FC)]
    xg[g_me] = xt[c]
    arrived(xg.at[g_pa], xsem.at[48])

    def zof(k):
        return (z + OFFS[k] + NZ) % NZ

    def xsend(k):
        zk = zof(k)
        for i, (s, g) in enumerate(((xt.at[c, zk], g_me), (xg.at[g_pa, zk], g_pa))):
            send(s, xg.at[g, zk], xsem.at[k * 6 + i], up)
            send(s, xg.at[g, zk], xsem.at[k * 6 + 2 + i], down)

    def xforward(k):
        zk = zof(k)
        for i in range(2):
            g_d, g_u = ym * 2 + (c if i == 0 else 1 - c), yp * 2 + (c if i == 0 else 1 - c)
            arrived(xg.at[g_d, zk], xsem.at[k * 6 + i])
            arrived(xg.at[g_u, zk], xsem.at[k * 6 + 2 + i])
        send(xg.at[ym * 2 + c, zk], xg.at[ym * 2 + c, zk], xsem.at[k * 6 + 4], up)
        send(xg.at[yp * 2 + 1 - c, zk], xg.at[yp * 2 + 1 - c, zk], xsem.at[k * 6 + 5], down)

    xsend(0)
    arrived(rel.at[0], dsem.at[0])
    send(rel.at[0], dyg.at[ym * 2 + c, 0], dsem.at[8], up)
    arrived(rel.at[1], dsem.at[1])
    send(rel.at[1], dyg.at[yp * 2 + c, 1], dsem.at[9], down)
    xsend(1)
    gd, gu, gf = ym * 2 + c, yp * 2 + c, y2 * 2 + c
    for n, (g, j, s) in enumerate(((gd, 0, 2), (gu, 0, 4), (gd, 1, 3), (gu, 1, 5))):
        arrived(dyg.at[g, j], dsem.at[s])
        send(dyg.at[g, j], dyg.at[g, j], dsem.at[10 + n], partner)
    xforward(0)
    for n, (g, j, s) in enumerate(((gf, 0, 8), (gf, 1, 9))):
        arrived(dyg.at[g, j], dsem.at[s])
        send(dyg.at[g, j], dyg.at[g, j], dsem.at[14 + n], partner)
    pd, pu, pf = ym * 2 + 1 - c, yp * 2 + 1 - c, y2 * 2 + 1 - c
    for g, j, s in ((g_pa, 0, 6), (g_pa, 1, 7), (pd, 0, 10), (pu, 0, 11), (pd, 1, 12), (pu, 1, 13), (pf, 0, 14), (pf, 1, 15)):
        arrived(dyg.at[g, j], dsem.at[s])

    def multiply(k, b, hh):
        zk = zof(k)
        for j in range(2):
            part[b, hh * 2 + j] = jnp.zeros((NE * HR, FC), jnp.float32)

        def step(g, _):
            v = xg[g, zk, hh]
            m = msk[g]
            lhs = jnp.concatenate([v * m[e:e + 1, :] for e in range(NE)], axis=0)
            for j in range(2):
                part[b, hh * 2 + j] += jnp.dot(lhs, dyg[g, j], preferred_element_type=jnp.float32)
            return 0
        lax.fori_loop(0, NG, step, 0)

    def rows(b, x_, h):
        return lambda e: part[b, x_, (h * HALF + e) * HR:(h * HALF + e + 1) * HR, :]

    def plus(*gets):
        return lambda e: functools.reduce(lambda p, q: p + q, [g(e) for g in gets])

    def compute(k):
        b = k % 3
        multiply(k, b, 1 - xh)
        opp = (X + 2) % NX
        encode(xa_s.at[k, 0], scales, rows(b, opp, 0))
        send(xa_s.at[k, 0], xa_r.at[k, 0], asem.at[k * 2], right)
        encode(xa_s.at[k, 1], scales, rows(b, opp, 1))
        send(xa_s.at[k, 1], xa_r.at[k, 1], asem.at[k * 2 + 1], left)
        multiply(k, b, xh)
        encode(xb_s.at[k, 0, 1], scales, rows(b, xp, 1))
        send(xb_s.at[k, 0, 1], xb_r.at[k, 0, 1], bsem.at[k * 4 + 1], right)
        encode(xb_s.at[k, 1, 0], scales, rows(b, xm, 0))
        send(xb_s.at[k, 1, 0], xb_r.at[k, 1, 0], bsem.at[k * 4 + 2], left)

    def xsum(k):
        b = k % 3
        arrived(xa_r.at[k, 0], asem.at[k * 2])
        encode(xb_s.at[k, 0, 0], scales, plus(rows(b, xp, 0), decoder(xa_r.at[k, 0])))
        send(xb_s.at[k, 0, 0], xb_r.at[k, 0, 0], bsem.at[k * 4], right)
        arrived(xa_r.at[k, 1], asem.at[k * 2 + 1])
        encode(xb_s.at[k, 1, 1], scales, plus(rows(b, xm, 1), decoder(xa_r.at[k, 1])))
        send(xb_s.at[k, 1, 1], xb_r.at[k, 1, 1], bsem.at[k * 4 + 3], left)

    def zsum(k):
        b, off = k % 3, OFFS[k]
        for i in range(2):
            for h in range(2):
                arrived(xb_r.at[k, i, h], bsem.at[k * 4 + i * 2 + h])
        terms = []
        for h in range(2):
            terms.append([rows(b, X, h), decoder(xb_r.at[k, 0, h]), decoder(xb_r.at[k, 1, h])])
        if off == 3:
            arrived(z_r.at[k, 0, 0], zsem.at[k * 2])
            terms[0].append(decoder(z_r.at[k, 0, 0]))
        elif off == -3:
            arrived(z_r.at[k, 1, 1], zsem.at[k * 2 + 1])
            terms[1].append(decoder(z_r.at[k, 1, 1]))
        else:
            for i in range(2):
                if (i == 0 and off in (2, 1, 0)) or (i == 1 and off in (-2, -1, 0)):
                    arrived(z_r.at[k, i], zsem.at[k * 2 + i])
                    for h in range(2):
                        terms[h].append(decoder(z_r.at[k, i, h]))
        if off == 0:
            for h in range(2):
                get = plus(*terms[h])
                for e in range(HALF):
                    out[h * HALF + e] = get(e)
            return
        for h in range(2):
            encode(z_s.at[k, h], scales, plus(*terms[h]))
        if off == 4:
            send(z_s.at[k, 0], z_r.at[1, 0, 0], zsem.at[1 * 2], ahead)
            send(z_s.at[k, 1], z_r.at[2, 1, 1], zsem.at[2 * 2 + 1], behind)
        elif off > 0:
            n = OFFS.index(off - 1)
            send(z_s.at[k], z_r.at[n, 0], zsem.at[n * 2], ahead)
        else:
            n = OFFS.index(off + 1)
            send(z_s.at[k], z_r.at[n, 1], zsem.at[n * 2 + 1], behind)

    for k in range(NZ):
        if k + 2 < NZ:
            xsend(k + 2)
        if k + 1 < NZ:
            xforward(k + 1)
        zk = zof(k)
        arrived(xg.at[y2 * 2 + c, zk], xsem.at[k * 6 + 4])
        arrived(xg.at[y2 * 2 + 1 - c, zk], xsem.at[k * 6 + 5])
        compute(k)
        if k >= 1:
            xsum(k - 1)
        if k >= 2:
            zsum(k - 2)
    xsum(NZ - 1)
    zsum(NZ - 2)
    zsum(NZ - 1)
    for op in started:
        op.wait_send()


def shards(x_rows, dy_rows, seg_blocks):
    rows, hid = x_rows.shape
    nblk = rows // BLOCK
    dp, ex = lax.axis_index("dp"), lax.axis_index("expert")
    g = jnp.arange(NG)
    devices = ((dp // 2) * 2 + g % 2) * NG + (ex // NY) * NY + g // 2
    ends = jnp.cumsum(seg_blocks[devices], axis=1)
    block = jnp.arange(nblk, dtype=jnp.int32)
    owner = jnp.sum((ends[:, None, :] <= block[None, :, None]).astype(jnp.int32), axis=2)
    mask = (owner[:, None, :] == jnp.arange(NE)[None, :, None]).astype(x_rows.dtype)
    mask = jnp.repeat(mask, BLOCK, axis=2)
    xt = x_rows.T.reshape(NZ, 2, 2, HR, rows).transpose(2, 0, 1, 3, 4)
    vm = pl.BlockSpec(memory_space=pltpu.VMEM)
    i16 = jnp.int16
    return pl.pallas_call(
        kernel,
        out_shape=jax.ShapeDtypeStruct((NE, HR, FC), jnp.float32),
        in_specs=[vm] * 3,
        out_specs=vm,
        scratch_shapes=[
            pltpu.VMEM((NG, NZ, 2, HR, rows), x_rows.dtype),
            pltpu.VMEM((NG, 2, rows, FC), x_rows.dtype),
            pltpu.VMEM((2, rows, FC), x_rows.dtype),
            pltpu.VMEM((3, 4, NE * HR, FC), jnp.float32),
            pltpu.VMEM((NZ, 2, MSG, FC), i16),
            pltpu.VMEM((NZ, 2, MSG, FC), i16),
            pltpu.VMEM((NZ, 2, 2, MSG, FC), i16),
            pltpu.VMEM((NZ, 2, 2, MSG, FC), i16),
            pltpu.VMEM((NZ, 2, MSG, FC), i16),
            pltpu.VMEM((NZ, 2, 2, MSG, FC), i16),
            pltpu.VMEM((16, FC), jnp.float32),
            pltpu.SemaphoreType.DMA((16, 2)),
            pltpu.SemaphoreType.DMA((49, 2)),
            pltpu.SemaphoreType.DMA((16, 2)),
            pltpu.SemaphoreType.DMA((32, 2)),
            pltpu.SemaphoreType.DMA((16, 2)),
        ],
        compiler_params=pltpu.CompilerParams(
            collective_id=0, has_side_effects=True, vmem_limit_bytes=56 << 20),
    )(xt, dy_rows, mask)


def solution(mesh):
    in_specs = (P(("dp", "expert"), None), P(("dp", "expert"), None), P())
    out_specs = P(None, "dp", "expert")
    return jax.shard_map(shards, mesh=mesh, in_specs=in_specs, out_specs=out_specs, check_vma=False)
```

```python
import functools

import jax
import jax.numpy as jnp
from jax import lax
from jax.experimental import pallas as pl
from jax.experimental.pallas import tpu as pltpu
from jax.sharding import PartitionSpec as P

BLOCK = 128
NE = 8
NC = NE - 1
NB = (4, 3)
TOK = 2 * BLOCK
NY, NX, NZ = 4, 4, 8
NG = 2 * NY
GG = 4
HR, FC = 32, 256
MSG = 4 * HR + 16
OFFS = (4, 3, -3, 2, -2, 1, -1, 0)
QMAX = 32700.0


def encode(dst, scales, n, get):
    for e in range(n):
        v = get(e)
        top = jnp.max(jnp.abs(v), axis=0, keepdims=True)
        lev = jnp.ceil(jnp.log2(jnp.maximum(top, 1e-30)) * 256.0) + 1.0
        q = jnp.round(v * (jnp.exp2(lev * (-1.0 / 256.0)) * QMAX))
        dst[e * HR:(e + 1) * HR, :] = q.astype(jnp.int32).astype(jnp.int16)
        scales[e:e + 1, :] = lev
    dst[n * HR:n * HR + 16, :] = scales[...].astype(jnp.int32).astype(jnp.int16)


def decoder(src, n):
    lev = src[n * HR:n * HR + 16, :].astype(jnp.int32).astype(jnp.float32)
    s = jnp.exp2(lev * (1.0 / 256.0)) * (1.0 / QMAX)

    def get(e):
        q = src[e * HR:(e + 1) * HR, :].astype(jnp.int32).astype(jnp.float32)
        return q * s[e:e + 1, :]
    return get


def plus(*gets):
    return lambda e: functools.reduce(lambda p, q: p + q, [g(e) for g in gets])


def span(n):
    return pl.ds(0, n * HR + 16)


def kernel(pos, x, dy, msk, out, xo_h, xo_c, xh_p, xg, dyh_o, dyh_p, dyc, dyg, rel, lhs, part, hp, xa_s, xa_r, xb_s, xb_r,
           z_s, z_r, hz_s, hz_r, hr, hxa_s, hxa_r, hxb_s, hxb_r, hy, hy_s, hy_r, scales,
           dsem, xsem, asem, bsem, zsem, hsem, tsem):
    dp, ex = lax.axis_index("dp"), lax.axis_index("expert")
    z, xh, c = dp // 4, (dp // 2) % 2, dp % 2
    xl, y = ex // NY, ex % NY
    X = xh * 2 + xl

    def at(z_=z, x_=X, c_=c, y_=y):
        return (z_ * 4 + (x_ // 2) * 2 + c_, (x_ % 2) * NY + y_)

    yp, ym, y2 = (y + 1) % NY, (y + 3) % NY, (y + 2) % NY
    xp, xm, x2 = (X + 1) % NX, (X + 3) % NX, (X + 2) % NX
    zp, zm = (z + 1) % NZ, (z + 7) % NZ
    partner = at(c_=1 - c)
    up, down = at(y_=yp), at(y_=ym)
    right, left = at(x_=xp), at(x_=xm)
    ahead, behind = at(z_=zp), at(z_=zm)
    g_me, g_pa = y * 2 + c, y * 2 + 1 - c

    barrier = pltpu.get_barrier_semaphore()
    for other in (partner, up, down, right, left, ahead, behind):
        pl.semaphore_signal(barrier, inc=1, device_id=other, device_id_type=pl.DeviceIdType.MESH)
    scales[...] = jnp.zeros_like(scales)

    def pick(ref, j, i, n):
        a, b = ref[j * BLOCK:(j + 1) * BLOCK, n], ref[(j + 2) * BLOCK:(j + 3) * BLOCK, n]
        m = 2 * j + 1 - i
        return a * pos[m:m + 1, n] + b * pos[2 * j + i:2 * j + i + 1, n]

    for i, dst in ((1, dyc), (0, dyh_o)):
        for j in range(2):
            dst[j * BLOCK:(j + 1) * BLOCK, :] = pick(dy, j, i, slice(0, 8 * FC))
    pl.semaphore_wait(barrier, 7)

    started = []

    def copy(src, dst, sem, dev):
        return pltpu.make_async_remote_copy(
            src_ref=src, dst_ref=dst, send_sem=sem.at[0], recv_sem=sem.at[1],
            device_id=dev, device_id_type=pl.DeviceIdType.MESH)

    def send(src, dst, sem, dev):
        op = copy(src, dst, sem, dev)
        op.start()
        started.append(op)

    def arrived(dst, sem):
        copy(dst, dst, sem, partner).wait_recv()

    def cols(yy, j):
        return pl.ds(pl.multiple_of((j * NY + yy) * FC, FC), FC)

    def dyslot(j, g):
        return dyg.at[j, pl.ds(pl.multiple_of(g * TOK, TOK), TOK)]

    send(dyc.at[:, cols(y2, 0)], rel.at[0], dsem.at[0], up)
    send(dyc.at[:, cols(y2, 1)], rel.at[1], dsem.at[1], down)
    send(dyh_o, dyh_p, tsem.at[0], partner)
    for j in range(2):
        send(dyc.at[:, cols(yp, j)], dyslot(j, g_me), dsem.at[2 + j], up)
        send(dyc.at[:, cols(ym, j)], dyslot(j, g_me), dsem.at[4 + j], down)
        send(dyc.at[:, cols(y, j)], dyslot(j, g_me), dsem.at[6 + j], partner)
    for j in range(2):
        dyg[j, pl.ds(pl.multiple_of(g_me * TOK, TOK), TOK)] = dyc[:, cols(y, j)]

    def turn(n, _):
        for j in range(4):
            t = pick(x, j % 2, j // 2, pl.ds(pl.multiple_of(n * BLOCK, BLOCK), BLOCK)).T
            dst = (xo_h, xo_c)[j // 2]
            for i in range(4):
                dst[i % 2, n, i // 2, :, (j % 2) * BLOCK:(j % 2 + 1) * BLOCK] = t[i * HR:(i + 1) * HR, :]
        return 0
    lax.fori_loop(0, NZ, turn, 0)
    send(xo_h.at[1 - c], xh_p, tsem.at[1], partner)
    send(xo_c.at[1 - c], xg.at[g_me], tsem.at[2], partner)
    xg[g_me] = xo_c[c]

    def zof(k):
        return (z + OFFS[k] + NZ) % NZ

    def xsend(k):
        zk = zof(k)
        for i, (s, g) in enumerate(((xo_c.at[c, zk], g_me), (xg.at[g_pa, zk], g_pa))):
            send(s, xg.at[g, zk], xsem.at[k * 6 + i], up)
            send(s, xg.at[g, zk], xsem.at[k * 6 + 2 + i], down)

    def xforward(k):
        zk = zof(k)
        for i in range(2):
            g_d, g_u = ym * 2 + (c if i == 0 else 1 - c), yp * 2 + (c if i == 0 else 1 - c)
            arrived(xg.at[g_d, zk], xsem.at[k * 6 + i])
            arrived(xg.at[g_u, zk], xsem.at[k * 6 + 2 + i])
        send(xg.at[ym * 2 + c, zk], xg.at[ym * 2 + c, zk], xsem.at[k * 6 + 4], up)
        send(xg.at[yp * 2 + 1 - c, zk], xg.at[yp * 2 + 1 - c, zk], xsem.at[k * 6 + 5], down)

    def hmultiply():
        left_ = jnp.concatenate([xo_h[c].reshape(NZ * 2 * HR, TOK), xh_p[...].reshape(NZ * 2 * HR, TOK)], axis=1)
        for n in range(8):
            r = jnp.concatenate([dyh_o[:, n * FC:(n + 1) * FC], dyh_p[:, n * FC:(n + 1) * FC]], axis=0)
            hp[n] = jnp.dot(left_, r, preferred_element_type=jnp.float32).reshape(NZ, 2, HR, FC)

    def hrows(k, u):
        zk = zof(k)
        return lambda i: hp[(u % 2) * NY + i, zk, u // 2]

    def hstart():
        for u, n, i, dev in ((0, 1, 0, ahead), (2, 2, 1, behind), (1, 1, 0, ahead), (3, 2, 1, behind)):
            encode(hz_s.at[0, u], scales, 4, hrows(0, u))
            send(hz_s.at[0, u], hz_r.at[n, i, u], hsem.at[(n * 2 + i) * 4 + u], dev)

    def hstep(off):
        for t in range(4):
            for i, dev in ((0, ahead), (1, behind)):
                k = OFFS.index(off if i == 0 else -off)
                n = OFFS.index(off - 1 if i == 0 else 1 - off)
                u = ((2, 3, 0, 1) if i == 0 else (0, 1, 2, 3))[t]
                get = hrows(k, u)
                if off < 3 or t >= 2:
                    arrived(hz_r.at[k, i, u], hsem.at[(k * 2 + i) * 4 + u])
                    get = plus(get, decoder(hz_r.at[k, i, u], 4))
                encode(hz_s.at[k, u], scales, 4, get)
                send(hz_s.at[k, u], hz_r.at[n, i, u], hsem.at[(n * 2 + i) * 4 + u], dev)

    def hlast():
        for u in range(4):
            for i in range(2):
                arrived(hz_r.at[7, i, u], hsem.at[(7 * 2 + i) * 4 + u])
            get = plus(hrows(7, u), decoder(hz_r.at[7, 0, u], 4), decoder(hz_r.at[7, 1, u], 4))
            for i in range(4):
                hr[u, i] = get(i)
        encode(hxa_s.at[0], scales, 2, lambda i: hr[x2, i])
        send(hxa_s.at[0, span(2)], hxa_r.at[0, span(2)], tsem.at[3], right)
        encode(hxa_s.at[1], scales, 2, lambda i: hr[x2, 2 + i])
        send(hxa_s.at[1, span(2)], hxa_r.at[1, span(2)], tsem.at[4], left)

    def hx():
        arrived(hxa_r.at[0, span(2)], tsem.at[3])
        arrived(hxa_r.at[1, span(2)], tsem.at[4])
        d0, d1 = decoder(hxa_r.at[0], 2), decoder(hxa_r.at[1], 2)
        encode(hxb_s.at[0], scales, 4, lambda i: hr[xp, i] + d0(i) if i < 2 else hr[xp, i])
        send(hxb_s.at[0], hxb_r.at[0], tsem.at[5], right)
        encode(hxb_s.at[1], scales, 4, lambda i: hr[xm, i] + d1(i - 2) if i >= 2 else hr[xm, i])
        send(hxb_s.at[1], hxb_r.at[1], tsem.at[6], left)

    def hxlast():
        arrived(hxb_r.at[0], tsem.at[5])
        arrived(hxb_r.at[1], tsem.at[6])
        get = plus(lambda i: hr[X, i], decoder(hxb_r.at[0], 4), decoder(hxb_r.at[1], 4))
        for i in range(4):
            hy[i] = get(i)
        send(hy.at[y2], hy_r.at[0], tsem.at[7], up)
        send(hy.at[ym], hy_r.at[2], tsem.at[8], down)

    def hyadd():
        arrived(hy_r.at[0], tsem.at[7])
        hy_s[...] = hy[yp] + hy_r[0]
        send(hy_s, hy_r.at[1], tsem.at[9], up)

    def hylast():
        arrived(hy_r.at[2], tsem.at[8])
        arrived(hy_r.at[1], tsem.at[9])
        out[0] = hy[y] + hy_r[1] + hy_r[2]

    def multiply(k):
        b, zk = k % 3, zof(k)
        for q in range(NG // GG):
            for h in range(2):
                v = jnp.concatenate([xg[q * GG + i, zk, h] for i in range(GG)], axis=1)
                for e in range(NC):
                    lhs[(h * NC + e) * HR:(h * NC + e + 1) * HR, :] = v * msk[q, e:e + 1, :]
            for j in range(2):
                r = jnp.dot(lhs[...], dyg[j, q * GG * TOK:(q + 1) * GG * TOK, :], preferred_element_type=jnp.float32)
                r = r.reshape(2, NC * HR, FC)
                part[b, j] = r if q == 0 else part[b, j] + r

    def rows(k, x_, h):
        return lambda e: part[k % 3, x_ % 2, x_ // 2, (h * 4 + e) * HR:(h * 4 + e + 1) * HR, :]

    def compute(k):
        multiply(k)
        for h, dev in ((0, right), (1, left)):
            encode(xa_s.at[k, h], scales, NB[h], rows(k, x2, h))
            send(xa_s.at[k, h, span(NB[h])], xa_r.at[k, h, span(NB[h])], asem.at[k * 2 + h], dev)
        for i, h, x_, dev in ((0, 1, xp, right), (1, 0, xm, left)):
            encode(xb_s.at[k, i, h], scales, NB[h], rows(k, x_, h))
            send(xb_s.at[k, i, h, span(NB[h])], xb_r.at[k, i, h, span(NB[h])], bsem.at[k * 4 + i * 2 + h], dev)

    def xsum(k):
        for h, x_, dev in ((0, xp, right), (1, xm, left)):
            arrived(xa_r.at[k, h, span(NB[h])], asem.at[k * 2 + h])
            encode(xb_s.at[k, h, h], scales, NB[h], plus(rows(k, x_, h), decoder(xa_r.at[k, h], NB[h])))
            send(xb_s.at[k, h, h, span(NB[h])], xb_r.at[k, h, h, span(NB[h])], bsem.at[k * 4 + h * 2 + h], dev)

    def zsum(k):
        off = OFFS[k]
        for h in range(2):
            n = NB[h]
            for i in range(2):
                arrived(xb_r.at[k, i, h, span(n)], bsem.at[k * 4 + i * 2 + h])
            terms = [rows(k, X, h), decoder(xb_r.at[k, 0, h], n), decoder(xb_r.at[k, 1, h], n)]
            for i in range(2):
                sign = off if i == 0 else -off
                if sign in (0, 1, 2) or (sign == 3 and h == i):
                    arrived(z_r.at[k, i, h, span(n)], zsem.at[(k * 2 + i) * 2 + h])
                    terms.append(decoder(z_r.at[k, i, h], n))
            get = plus(*terms)
            if off == 0:
                for e in range(n):
                    out[1 + h * 4 + e] = get(e)
                continue
            encode(z_s.at[k, h], scales, n, get)
            i = h if off == 4 else (0 if off > 0 else 1)
            m = OFFS.index((3, -3)[i] if off == 4 else (off - 1 if off > 0 else off + 1))
            send(z_s.at[k, h, span(n)], z_r.at[m, i, h, span(n)], zsem.at[(m * 2 + i) * 2 + h], (ahead, behind)[i])

    arrived(rel.at[0], dsem.at[0])
    send(rel.at[0], dyslot(0, ym * 2 + c), dsem.at[8], up)
    arrived(rel.at[1], dsem.at[1])
    send(rel.at[1], dyslot(1, yp * 2 + c), dsem.at[9], down)
    arrived(xg.at[g_pa], tsem.at[2])
    xsend(0)
    xsend(1)
    arrived(xh_p, tsem.at[1])
    arrived(dyh_p, tsem.at[0])
    hmultiply()
    hstart()
    gd, gu, gf = ym * 2 + c, yp * 2 + c, y2 * 2 + c
    for n, (g, j, s) in enumerate(((gd, 0, 2), (gu, 0, 4), (gd, 1, 3), (gu, 1, 5))):
        arrived(dyslot(j, g), dsem.at[s])
        send(dyslot(j, g), dyslot(j, g), dsem.at[10 + n], partner)
    hstep(3)
    for n, (g, j, s) in enumerate(((gf, 0, 8), (gf, 1, 9))):
        arrived(dyslot(j, g), dsem.at[s])
        send(dyslot(j, g), dyslot(j, g), dsem.at[14 + n], partner)
    xforward(0)
    pd, pu, pf = ym * 2 + 1 - c, yp * 2 + 1 - c, y2 * 2 + 1 - c
    for g, j, s in ((g_pa, 0, 6), (g_pa, 1, 7), (pd, 0, 10), (pu, 0, 11), (pd, 1, 12), (pu, 1, 13), (pf, 0, 14), (pf, 1, 15)):
        arrived(dyslot(j, g), dsem.at[s])

    for k in range(NZ):
        if k + 2 < NZ:
            xsend(k + 2)
        if k + 1 < NZ:
            xforward(k + 1)
        zk = zof(k)
        arrived(xg.at[y2 * 2 + c, zk], xsem.at[k * 6 + 4])
        arrived(xg.at[y2 * 2 + 1 - c, zk], xsem.at[k * 6 + 5])
        compute(k)
        if k >= 1:
            xsum(k - 1)
        if k >= 2:
            zsum(k - 2)
        if k == 0:
            hstep(2)
        elif k == 2:
            hstep(1)
        elif k == 3:
            hlast()
        elif k == 4:
            hx()
        elif k == 5:
            hxlast()
        elif k == 6:
            hyadd()
    xsum(NZ - 1)
    zsum(NZ - 2)
    hylast()
    zsum(NZ - 1)
    for op in started:
        op.wait_send()


def shards(x_rows, dy_rows, seg_blocks):
    dp, ex = lax.axis_index("dp"), lax.axis_index("expert")
    bf16, f32, i16 = jnp.bfloat16, jnp.float32, jnp.int16
    i32 = jnp.int32
    hot = jnp.argmax(jnp.all(seg_blocks == 2, axis=0)).astype(i32)
    g = jnp.arange(NG, dtype=i32)
    devices = ((dp // 2) * 2 + g % 2) * NG + (ex // NY) * NY + g // 2
    counts = seg_blocks[devices]
    ends = jnp.cumsum(counts, axis=1)
    first = jnp.sum(jnp.where(jnp.arange(NE)[None, :] < hot, counts, 0), axis=1)
    slot = jnp.arange(2, dtype=i32)[None, :]
    cold = jnp.where(slot < first[:, None], slot, slot + 2)
    owner = jnp.sum((ends[:, None, :] <= cold[:, :, None]).astype(i32), axis=2)
    r = jnp.arange(NC, dtype=i32)
    names = r + (r >= hot).astype(i32)
    mask = jnp.repeat((owner[:, None, :] == names[None, :, None]).astype(bf16), BLOCK, axis=2)
    mask = mask.reshape(NG // GG, GG, NC, TOK).transpose(0, 2, 1, 3).reshape(NG // GG, NC, GG * TOK)
    me = (ex % NY) * 2 + dp % 2
    low = slot[0] < first[me]
    pos = jnp.broadcast_to(jnp.stack([low, ~low], axis=1).reshape(4, 1).astype(bf16), (4, 8 * FC))
    vm = pl.BlockSpec(memory_space=pltpu.VMEM)
    sem = pltpu.SemaphoreType.DMA
    res = pl.pallas_call(
        kernel,
        out_shape=jax.ShapeDtypeStruct((NE, HR, FC), f32),
        in_specs=[vm] * 4,
        out_specs=vm,
        scratch_shapes=[
            pltpu.VMEM((2, NZ, 2, HR, TOK), bf16),
            pltpu.VMEM((2, NZ, 2, HR, TOK), bf16),
            pltpu.VMEM((NZ, 2, HR, TOK), bf16),
            pltpu.VMEM((NG, NZ, 2, HR, TOK), bf16),
            pltpu.VMEM((TOK, 8 * FC), bf16),
            pltpu.VMEM((TOK, 8 * FC), bf16),
            pltpu.VMEM((TOK, 8 * FC), bf16),
            pltpu.VMEM((2, NG * TOK, FC), bf16),
            pltpu.VMEM((2, TOK, FC), bf16),
            pltpu.VMEM((2 * NC * HR, GG * TOK), bf16),
            pltpu.VMEM((3, 2, 2, NC * HR, FC), f32),
            pltpu.VMEM((8, NZ, 2, HR, FC), f32),
            pltpu.VMEM((NZ, 2, MSG, FC), i16),
            pltpu.VMEM((NZ, 2, MSG, FC), i16),
            pltpu.VMEM((NZ, 2, 2, MSG, FC), i16),
            pltpu.VMEM((NZ, 2, 2, MSG, FC), i16),
            pltpu.VMEM((NZ, 2, MSG, FC), i16),
            pltpu.VMEM((NZ, 2, 2, MSG, FC), i16),
            pltpu.VMEM((NZ, 4, MSG, FC), i16),
            pltpu.VMEM((NZ, 2, 4, MSG, FC), i16),
            pltpu.VMEM((4, 4, HR, FC), f32),
            pltpu.VMEM((2, MSG, FC), i16),
            pltpu.VMEM((2, MSG, FC), i16),
            pltpu.VMEM((2, MSG, FC), i16),
            pltpu.VMEM((2, MSG, FC), i16),
            pltpu.VMEM((4, HR, FC), f32),
            pltpu.VMEM((HR, FC), f32),
            pltpu.VMEM((3, HR, FC), f32),
            pltpu.VMEM((16, FC), f32),
            sem((16, 2)), sem((48, 2)), sem((16, 2)), sem((32, 2)), sem((32, 2)), sem((64, 2)), sem((10, 2)),
        ],
        compiler_params=pltpu.CompilerParams(
            collective_id=0, has_side_effects=True, vmem_limit_bytes=58 << 20),
    )(pos, x_rows, dy_rows, mask)
    e = jnp.arange(NE, dtype=i32)
    return res[jnp.where(e == hot, 0, 1 + e - (e > hot).astype(i32))]


def solution(mesh):
    in_specs = (P(("dp", "expert"), None), P(("dp", "expert"), None), P())
    out_specs = P(None, "dp", "expert")
    return jax.shard_map(shards, mesh=mesh, in_specs=in_specs, out_specs=out_specs, check_vma=False)
```

```python
import functools

import jax
import jax.numpy as jnp
from jax import lax
from jax.experimental import pallas as pl
from jax.experimental.pallas import tpu as pltpu
from jax.sharding import PartitionSpec as P

BLOCK = 128
NE = 8
NC = NE - 1
NX1 = 5
NB = (3, 2)
TOK = 2 * BLOCK
NY, NX, NZ = 4, 4, 8
NG = 2 * NY
GG = 4
HR, FC = 32, 256
MSG = 4 * HR + 16
OFFS = (4, 3, -3, 2, -2, 1, -1, 0)
QMAX = 32700.0


def encode(dst, scales, n, get):
    for e in range(n):
        v = get(e)
        top = jnp.max(jnp.abs(v), axis=0, keepdims=True)
        lev = jnp.ceil(jnp.log2(jnp.maximum(top, 1e-30)) * 256.0) + 1.0
        q = jnp.round(v * (jnp.exp2(lev * (-1.0 / 256.0)) * QMAX))
        dst[e * HR:(e + 1) * HR, :] = q.astype(jnp.int32).astype(jnp.int16)
        scales[e:e + 1, :] = lev
    dst[n * HR:n * HR + 16, :] = scales[...].astype(jnp.int32).astype(jnp.int16)


def decoder(src, n):
    lev = src[n * HR:n * HR + 16, :].astype(jnp.int32).astype(jnp.float32)
    s = jnp.exp2(lev * (1.0 / 256.0)) * (1.0 / QMAX)

    def get(e):
        q = src[e * HR:(e + 1) * HR, :].astype(jnp.int32).astype(jnp.float32)
        return q * s[e:e + 1, :]
    return get


def plus(*gets):
    return lambda e: functools.reduce(lambda p, q: p + q, [g(e) for g in gets])


def span(n):
    return pl.ds(0, n * HR + 16)


def flag(cond):
    return jnp.where(cond, 1.0, 0.0).astype(jnp.float32)


def kernel(seg, segv, x_any, dy_any, out, x, dy, msk, xo_h, xo_c, xh_p, xg, dyh_o, dyh_p, dyc, dyg, rel, lhs, part, hp, xa_s, xa_r, xb_s, xb_r,
           z_s, z_r, hz_s, hz_r, hr, hxa_s, hxa_r, hxb_s, hxb_r, hy, hy_s, hy_r, scales,
           cz_s, cz_r, cr, cxa_r, cx_s, cxb_r, res, dsem, xsem, asem, bsem, zsem, hsem, tsem, csem, cxsem, lsem):
    dp, ex = lax.axis_index("dp"), lax.axis_index("expert")
    z, xh, c = dp // 4, (dp // 2) % 2, dp % 2
    xl, y = ex // NY, ex % NY
    X = xh * 2 + xl

    def at(z_=z, x_=X, c_=c, y_=y):
        return (z_ * 4 + (x_ // 2) * 2 + c_, (x_ % 2) * NY + y_)

    yp, ym, y2 = (y + 1) % NY, (y + 3) % NY, (y + 2) % NY
    xp, xm, x2 = (X + 1) % NX, (X + 3) % NX, (X + 2) % NX
    zp, zm = (z + 1) % NZ, (z + 7) % NZ
    partner = at(c_=1 - c)
    up, down = at(y_=yp), at(y_=ym)
    right, left = at(x_=xp), at(x_=xm)
    ahead, behind = at(z_=zp), at(z_=zm)
    g_me, g_pa = y * 2 + c, y * 2 + 1 - c

    barrier = pltpu.get_barrier_semaphore()
    for other in (partner, up, down, right, left, ahead, behind):
        pl.semaphore_signal(barrier, inc=1, device_id=other, device_id_type=pl.DeviceIdType.MESH)
    load_dy = pltpu.make_async_copy(dy_any, dy, lsem.at[0])
    load_x = pltpu.make_async_copy(x_any, x, lsem.at[1])
    load_dy.start()
    load_x.start()
    scales[...] = jnp.zeros_like(scales)

    twos = jnp.min(jnp.where(segv[...] == 2, 1.0, 0.0), axis=1, keepdims=True)
    index = lax.broadcasted_iota(jnp.int32, (NE, 1), 0)
    hot = jnp.min(jnp.where(twos > 0.5, index, NE))

    def cold_blocks(g):
        device = ((dp // 2) * 2 + g % 2) * NG + xl * NY + g // 2
        ends, first, total = [], 0, 0
        for e in range(NE):
            n = seg[e, device]
            total = total + n
            ends.append(total)
            first = first + jnp.where(e < hot, n, 0)
        picked = []
        for j in range(2):
            low = j < first
            at_ = jnp.where(low, j, j + 2)
            owner = 0
            for e in range(NE):
                owner = owner + jnp.where(ends[e] <= at_, 1, 0)
            picked.append((low, owner))
        return picked

    for g in range(NG):
        for j, (_, owner) in enumerate(cold_blocks(g)):
            for e in range(NC):
                name = e + jnp.where(e >= hot, 1, 0)
                lanes = slice((g % GG) * TOK + j * BLOCK, (g % GG) * TOK + (j + 1) * BLOCK)
                msk[g // GG, e:e + 1, lanes] = jnp.full((1, BLOCK), flag(owner == name), jnp.float32)
    low = [flag(c_[0]) for c_ in cold_blocks(g_me)]

    def pick(ref, j, i, n, width):
        w = low[j] if i == 1 else 1.0 - low[j]
        a, b = ref[j * BLOCK:(j + 1) * BLOCK, n], ref[(j + 2) * BLOCK:(j + 3) * BLOCK, n]
        return (a * jnp.full((1, width), w, jnp.float32).astype(a.dtype)
                + b * jnp.full((1, width), 1.0 - w, jnp.float32).astype(b.dtype))

    load_dy.wait()
    for i, dst in ((1, dyc), (0, dyh_o)):
        for j in range(2):
            dst[j * BLOCK:(j + 1) * BLOCK, :] = pick(dy, j, i, slice(0, 8 * FC), 8 * FC)
    load_x.wait()
    pl.semaphore_wait(barrier, 7)

    started = []

    def copy(src, dst, sem, dev):
        return pltpu.make_async_remote_copy(
            src_ref=src, dst_ref=dst, send_sem=sem.at[0], recv_sem=sem.at[1],
            device_id=dev, device_id_type=pl.DeviceIdType.MESH)

    def send(src, dst, sem, dev):
        op = copy(src, dst, sem, dev)
        op.start()
        started.append(op)

    def arrived(dst, sem):
        copy(dst, dst, sem, partner).wait_recv()

    def cols(yy, j):
        return pl.ds(pl.multiple_of((j * NY + yy) * FC, FC), FC)

    def dyslot(j, g):
        return dyg.at[j, pl.ds(pl.multiple_of(g * TOK, TOK), TOK)]

    send(dyc.at[:, cols(y2, 0)], rel.at[0], dsem.at[0], up)
    send(dyc.at[:, cols(y2, 1)], rel.at[1], dsem.at[1], down)
    send(dyh_o, dyh_p, tsem.at[0], partner)
    for j in range(2):
        send(dyc.at[:, cols(yp, j)], dyslot(j, g_me), dsem.at[2 + j], up)
        send(dyc.at[:, cols(ym, j)], dyslot(j, g_me), dsem.at[4 + j], down)
        send(dyc.at[:, cols(y, j)], dyslot(j, g_me), dsem.at[6 + j], partner)
    for j in range(2):
        dyg[j, pl.ds(pl.multiple_of(g_me * TOK, TOK), TOK)] = dyc[:, cols(y, j)]

    def turn(n, _):
        for j in range(4):
            t = pick(x, j % 2, j // 2, pl.ds(pl.multiple_of(n * BLOCK, BLOCK), BLOCK), BLOCK).T
            dst = (xo_h, xo_c)[j // 2]
            for i in range(4):
                dst[i % 2, n, i // 2, :, (j % 2) * BLOCK:(j % 2 + 1) * BLOCK] = t[i * HR:(i + 1) * HR, :]
        return 0
    lax.fori_loop(0, NZ, turn, 0)
    send(xo_h.at[1 - c], xh_p, tsem.at[1], partner)
    send(xo_c.at[1 - c], xg.at[g_me], tsem.at[2], partner)
    xg[g_me] = xo_c[c]

    def zof(k):
        return (z + OFFS[k] + NZ) % NZ

    def xsend(k):
        zk = zof(k)
        for i, (s, g) in enumerate(((xo_c.at[c, zk], g_me), (xg.at[g_pa, zk], g_pa))):
            send(s, xg.at[g, zk], xsem.at[k * 6 + i], up)
            send(s, xg.at[g, zk], xsem.at[k * 6 + 2 + i], down)

    def xforward(k):
        zk = zof(k)
        for i in range(2):
            g_d, g_u = ym * 2 + (c if i == 0 else 1 - c), yp * 2 + (c if i == 0 else 1 - c)
            arrived(xg.at[g_d, zk], xsem.at[k * 6 + i])
            arrived(xg.at[g_u, zk], xsem.at[k * 6 + 2 + i])
        send(xg.at[ym * 2 + c, zk], xg.at[ym * 2 + c, zk], xsem.at[k * 6 + 4], up)
        send(xg.at[yp * 2 + 1 - c, zk], xg.at[yp * 2 + 1 - c, zk], xsem.at[k * 6 + 5], down)

    def hmultiply():
        left_ = jnp.concatenate([xo_h[c].reshape(NZ * 2 * HR, TOK), xh_p[...].reshape(NZ * 2 * HR, TOK)], axis=1)
        for n in range(8):
            r = jnp.concatenate([dyh_o[:, n * FC:(n + 1) * FC], dyh_p[:, n * FC:(n + 1) * FC]], axis=0)
            hp[n] = jnp.dot(left_, r, preferred_element_type=jnp.float32).reshape(NZ, 2, HR, FC)

    def hrows(k, u):
        zk = zof(k)
        return lambda i: hp[(u % 2) * NY + i, zk, u // 2]

    def hstart():
        for u, n, i, dev in ((0, 1, 0, ahead), (2, 2, 1, behind), (1, 1, 0, ahead), (3, 2, 1, behind)):
            encode(hz_s.at[0, u], scales, 4, hrows(0, u))
            send(hz_s.at[0, u], hz_r.at[n, i, u], hsem.at[(n * 2 + i) * 4 + u], dev)

    def hstep(off):
        for t in range(4):
            for i, dev in ((0, ahead), (1, behind)):
                k = OFFS.index(off if i == 0 else -off)
                n = OFFS.index(off - 1 if i == 0 else 1 - off)
                u = ((2, 3, 0, 1) if i == 0 else (0, 1, 2, 3))[t]
                get = hrows(k, u)
                if off < 3 or t >= 2:
                    arrived(hz_r.at[k, i, u], hsem.at[(k * 2 + i) * 4 + u])
                    get = plus(get, decoder(hz_r.at[k, i, u], 4))
                encode(hz_s.at[k, u], scales, 4, get)
                send(hz_s.at[k, u], hz_r.at[n, i, u], hsem.at[(n * 2 + i) * 4 + u], dev)

    def hlast():
        for u in range(4):
            for i in range(2):
                arrived(hz_r.at[7, i, u], hsem.at[(7 * 2 + i) * 4 + u])
            get = plus(hrows(7, u), decoder(hz_r.at[7, 0, u], 4), decoder(hz_r.at[7, 1, u], 4))
            for i in range(4):
                hr[u, i] = get(i)
        encode(hxa_s.at[0], scales, 2, lambda i: hr[x2, i])
        send(hxa_s.at[0, span(2)], hxa_r.at[0, span(2)], tsem.at[3], right)
        encode(hxa_s.at[1], scales, 2, lambda i: hr[x2, 2 + i])
        send(hxa_s.at[1, span(2)], hxa_r.at[1, span(2)], tsem.at[4], left)

    def hx():
        arrived(hxa_r.at[0, span(2)], tsem.at[3])
        arrived(hxa_r.at[1, span(2)], tsem.at[4])
        d0, d1 = decoder(hxa_r.at[0], 2), decoder(hxa_r.at[1], 2)
        encode(hxb_s.at[0], scales, 4, lambda i: hr[xp, i] + d0(i) if i < 2 else hr[xp, i])
        send(hxb_s.at[0], hxb_r.at[0], tsem.at[5], right)
        encode(hxb_s.at[1], scales, 4, lambda i: hr[xm, i] + d1(i - 2) if i >= 2 else hr[xm, i])
        send(hxb_s.at[1], hxb_r.at[1], tsem.at[6], left)

    def hxlast():
        arrived(hxb_r.at[0], tsem.at[5])
        arrived(hxb_r.at[1], tsem.at[6])
        get = plus(lambda i: hr[X, i], decoder(hxb_r.at[0], 4), decoder(hxb_r.at[1], 4))
        for i in range(4):
            hy[i] = get(i)
        send(hy.at[y2], hy_r.at[0], tsem.at[7], up)
        send(hy.at[ym], hy_r.at[2], tsem.at[8], down)

    def hyadd():
        arrived(hy_r.at[0], tsem.at[7])
        hy_s[...] = hy[yp] + hy_r[0]
        send(hy_s, hy_r.at[1], tsem.at[9], up)

    def hylast():
        arrived(hy_r.at[2], tsem.at[8])
        arrived(hy_r.at[1], tsem.at[9])
        res[0] = hy[y] + hy_r[1] + hy_r[2]

    def multiply(k):
        b, zk = k % 3, zof(k)
        for q in range(NG // GG):
            for h in range(2):
                v = jnp.concatenate([xg[q * GG + i, zk, h] for i in range(GG)], axis=1)
                for e in range(NC):
                    lhs[(h * NC + e) * HR:(h * NC + e + 1) * HR, :] = v * msk[q, e:e + 1, :].astype(v.dtype)
            for j in range(2):
                r = jnp.dot(lhs[...], dyg[j, q * GG * TOK:(q + 1) * GG * TOK, :], preferred_element_type=jnp.float32)
                r = r.reshape(2, NC * HR, FC)
                part[b, j] = r if q == 0 else part[b, j] + r

    def rows(k, x_, h):
        return lambda e: part[k % 3, x_ % 2, x_ // 2, (h * NB[0] + e) * HR:(h * NB[0] + e + 1) * HR, :]

    def compute(k):
        multiply(k)
        for h, dev in ((0, right), (1, left)):
            encode(xa_s.at[k, h], scales, NB[h], rows(k, x2, h))
            send(xa_s.at[k, h, span(NB[h])], xa_r.at[k, h, span(NB[h])], asem.at[k * 2 + h], dev)
        for i, h, x_, dev in ((0, 1, xp, right), (1, 0, xm, left)):
            encode(xb_s.at[k, i, h], scales, NB[h], rows(k, x_, h))
            send(xb_s.at[k, i, h, span(NB[h])], xb_r.at[k, i, h, span(NB[h])], bsem.at[k * 4 + i * 2 + h], dev)

    def xsum(k):
        for h, x_, dev in ((0, xp, right), (1, xm, left)):
            arrived(xa_r.at[k, h, span(NB[h])], asem.at[k * 2 + h])
            encode(xb_s.at[k, h, h], scales, NB[h], plus(rows(k, x_, h), decoder(xa_r.at[k, h], NB[h])))
            send(xb_s.at[k, h, h, span(NB[h])], xb_r.at[k, h, h, span(NB[h])], bsem.at[k * 4 + h * 2 + h], dev)

    def zsum(k):
        off = OFFS[k]
        for h in range(2):
            n = NB[h]
            for i in range(2):
                arrived(xb_r.at[k, i, h, span(n)], bsem.at[k * 4 + i * 2 + h])
            terms = [rows(k, X, h), decoder(xb_r.at[k, 0, h], n), decoder(xb_r.at[k, 1, h], n)]
            for i in range(2):
                sign = off if i == 0 else -off
                if sign in (0, 1, 2) or (sign == 3 and h == i):
                    arrived(z_r.at[k, i, h, span(n)], zsem.at[(k * 2 + i) * 2 + h])
                    terms.append(decoder(z_r.at[k, i, h], n))
            get = plus(*terms)
            if off == 0:
                for e in range(n):
                    res[1 + h * NB[0] + e] = get(e)
                continue
            encode(z_s.at[k, h], scales, n, get)
            i = h if off == 4 else (0 if off > 0 else 1)
            m = OFFS.index((3, -3)[i] if off == 4 else (off - 1 if off > 0 else off + 1))
            send(z_s.at[k, h, span(n)], z_r.at[m, i, h, span(n)], zsem.at[(m * 2 + i) * 2 + h], (ahead, behind)[i])

    def czrows(k, u):
        return lambda i: part[k % 3, i // 2, u, (NX1 + i % 2) * HR:(NX1 + i % 2 + 1) * HR, :]

    def czsum(k):
        off = OFFS[k]
        for u in range(2):
            terms = [czrows(k, u)]
            for i in range(2):
                sign = off if i == 0 else -off
                if sign in (0, 1, 2) or (sign == 3 and u == i):
                    arrived(cz_r.at[k, i, u], csem.at[(k * 2 + i) * 2 + u])
                    terms.append(decoder(cz_r.at[k, i, u], 4))
            get = plus(*terms)
            if off == 0:
                for i in range(4):
                    cr[u * 2 + i // 2, i % 2] = get(i)
                continue
            encode(cz_s.at[k, u], scales, 4, get)
            i = u if off == 4 else (0 if off > 0 else 1)
            m = OFFS.index((3, -3)[i] if off == 4 else (off - 1 if off > 0 else off + 1))
            send(cz_s.at[k, u], cz_r.at[m, i, u], csem.at[(m * 2 + i) * 2 + u], (ahead, behind)[i])

    def cxsend():
        for i, x_, dev in ((0, xp, right), (1, xm, left)):
            send(cr.at[x2, i], cxa_r.at[i], cxsem.at[i], dev)
            send(cr.at[x_, 1 - i], cxb_r.at[i, 1 - i], cxsem.at[2 + i * 2 + 1 - i], dev)

    def cxsum():
        for i, x_, dev in ((0, xp, right), (1, xm, left)):
            arrived(cxa_r.at[i], cxsem.at[i])
            cx_s[i] = cr[x_, i] + cxa_r[i]
            send(cx_s.at[i], cxb_r.at[i, i], cxsem.at[2 + i * 2 + i], dev)

    def cxlast():
        for i in range(2):
            for e in range(2):
                arrived(cxb_r.at[i, e], cxsem.at[2 + i * 2 + e])
        for e in range(2):
            res[1 + NX1 + e] = cr[X, e] + cxb_r[0, e] + cxb_r[1, e]

    arrived(xh_p, tsem.at[1])
    arrived(dyh_p, tsem.at[0])
    hmultiply()
    hstart()
    arrived(rel.at[0], dsem.at[0])
    send(rel.at[0], dyslot(0, ym * 2 + c), dsem.at[8], up)
    arrived(rel.at[1], dsem.at[1])
    send(rel.at[1], dyslot(1, yp * 2 + c), dsem.at[9], down)
    arrived(xg.at[g_pa], tsem.at[2])
    xsend(0)
    xsend(1)
    gd, gu, gf = ym * 2 + c, yp * 2 + c, y2 * 2 + c
    for n, (g, j, s) in enumerate(((gd, 0, 2), (gu, 0, 4), (gd, 1, 3), (gu, 1, 5))):
        arrived(dyslot(j, g), dsem.at[s])
        send(dyslot(j, g), dyslot(j, g), dsem.at[10 + n], partner)
    for n, (g, j, s) in enumerate(((gf, 0, 8), (gf, 1, 9))):
        arrived(dyslot(j, g), dsem.at[s])
        send(dyslot(j, g), dyslot(j, g), dsem.at[14 + n], partner)
    hstep(3)
    xforward(0)
    pd, pu, pf = ym * 2 + 1 - c, yp * 2 + 1 - c, y2 * 2 + 1 - c
    for g, j, s in ((g_pa, 0, 6), (g_pa, 1, 7), (pd, 0, 10), (pu, 0, 11), (pd, 1, 12), (pu, 1, 13), (pf, 0, 14), (pf, 1, 15)):
        arrived(dyslot(j, g), dsem.at[s])

    for k in range(NZ):
        if k + 2 < NZ:
            xsend(k + 2)
        if k + 1 < NZ:
            xforward(k + 1)
        zk = zof(k)
        arrived(xg.at[y2 * 2 + c, zk], xsem.at[k * 6 + 4])
        arrived(xg.at[y2 * 2 + 1 - c, zk], xsem.at[k * 6 + 5])
        compute(k)
        czsum(k)
        if k == NZ - 1:
            cxsend()
        if k >= 1:
            xsum(k - 1)
        if k >= 2:
            zsum(k - 2)
        if k == 0:
            hstep(2)
        elif k == 2:
            hstep(1)
        elif k == 3:
            hlast()
        elif k == 4:
            hx()
        elif k == 5:
            hxlast()
        elif k == 6:
            hyadd()
    cxsum()
    xsum(NZ - 1)
    zsum(NZ - 2)
    hylast()
    cxlast()
    zsum(NZ - 1)
    for e in range(NE):
        v = res[0] * flag(e == hot)
        if e < NC:
            v = v + res[1 + e] * flag(e < hot)
        if e > 0:
            v = v + res[e] * flag(e > hot)
        out[e] = v
    for op in started:
        op.wait_send()


def shards(x_rows, dy_rows, seg_blocks):
    bf16, f32, i16 = jnp.bfloat16, jnp.float32, jnp.int16
    vm = pl.BlockSpec(memory_space=pltpu.VMEM)
    sem = pltpu.SemaphoreType.DMA
    return pl.pallas_call(
        kernel,
        out_shape=jax.ShapeDtypeStruct((NE, HR, FC), f32),
        in_specs=[pl.BlockSpec(memory_space=pltpu.SMEM), vm] + [pl.BlockSpec(memory_space=pl.ANY)] * 2,
        out_specs=vm,
        scratch_shapes=[
            pltpu.VMEM(x_rows.shape, bf16),
            pltpu.VMEM(dy_rows.shape, bf16),
            pltpu.VMEM((NG // GG, NE, GG * TOK), f32),
            pltpu.VMEM((2, NZ, 2, HR, TOK), bf16),
            pltpu.VMEM((2, NZ, 2, HR, TOK), bf16),
            pltpu.VMEM((NZ, 2, HR, TOK), bf16),
            pltpu.VMEM((NG, NZ, 2, HR, TOK), bf16),
            pltpu.VMEM((TOK, 8 * FC), bf16),
            pltpu.VMEM((TOK, 8 * FC), bf16),
            pltpu.VMEM((TOK, 8 * FC), bf16),
            pltpu.VMEM((2, NG * TOK, FC), bf16),
            pltpu.VMEM((2, TOK, FC), bf16),
            pltpu.VMEM((2 * NC * HR, GG * TOK), bf16),
            pltpu.VMEM((3, 2, 2, NC * HR, FC), f32),
            pltpu.VMEM((8, NZ, 2, HR, FC), f32),
            pltpu.VMEM((NZ, 2, MSG, FC), i16),
            pltpu.VMEM((NZ, 2, MSG, FC), i16),
            pltpu.VMEM((NZ, 2, 2, MSG, FC), i16),
            pltpu.VMEM((NZ, 2, 2, MSG, FC), i16),
            pltpu.VMEM((NZ, 2, MSG, FC), i16),
            pltpu.VMEM((NZ, 2, 2, MSG, FC), i16),
            pltpu.VMEM((NZ, 4, MSG, FC), i16),
            pltpu.VMEM((NZ, 2, 4, MSG, FC), i16),
            pltpu.VMEM((4, 4, HR, FC), f32),
            pltpu.VMEM((2, MSG, FC), i16),
            pltpu.VMEM((2, MSG, FC), i16),
            pltpu.VMEM((2, MSG, FC), i16),
            pltpu.VMEM((2, MSG, FC), i16),
            pltpu.VMEM((4, HR, FC), f32),
            pltpu.VMEM((HR, FC), f32),
            pltpu.VMEM((3, HR, FC), f32),
            pltpu.VMEM((16, FC), f32),
            pltpu.VMEM((NZ, 2, MSG, FC), i16),
            pltpu.VMEM((NZ, 2, 2, MSG, FC), i16),
            pltpu.VMEM((4, 2, HR, FC), f32),
            pltpu.VMEM((2, HR, FC), f32),
            pltpu.VMEM((2, HR, FC), f32),
            pltpu.VMEM((2, 2, HR, FC), f32),
            pltpu.VMEM((NE, HR, FC), f32),
            sem((16, 2)), sem((48, 2)), sem((16, 2)), sem((32, 2)), sem((32, 2)), sem((64, 2)), sem((10, 2)),
            sem((32, 2)), sem((6, 2)), sem((2,)),
        ],
        compiler_params=pltpu.CompilerParams(
            collective_id=0, has_side_effects=True, vmem_limit_bytes=58 << 20),
    )(seg_blocks.T, seg_blocks.T, x_rows, dy_rows)


def solution(mesh):
    in_specs = (P(("dp", "expert"), None), P(("dp", "expert"), None), P())
    out_specs = P(None, "dp", "expert")
    return jax.shard_map(shards, mesh=mesh, in_specs=in_specs, out_specs=out_specs, check_vma=False)
```

```python
import functools

import jax
import jax.numpy as jnp
from jax import lax
from jax.experimental import pallas as pl
from jax.experimental.pallas import tpu as pltpu
from jax.sharding import PartitionSpec as P

BLOCK = 128
NE = 8
NC = NE - 1
NX1 = 5
NB = (3, 2)
TOK = 2 * BLOCK
NY, NX, NZ = 4, 4, 8
NG = 2 * NY
GG = 4
HR, FC = 32, 256
MSG = 4 * HR + 16
OFFS = (4, 3, -3, 2, -2, 1, -1, 0)
QMAX = 32700.0


def encode(dst, scales, n, get):
    for e in range(n):
        v = get(e)
        top = jnp.max(jnp.abs(v), axis=0, keepdims=True)
        lev = jnp.ceil(jnp.log2(jnp.maximum(top, 1e-30)) * 256.0) + 1.0
        q = jnp.round(v * (jnp.exp2(lev * (-1.0 / 256.0)) * QMAX))
        dst[e * HR:(e + 1) * HR, :] = q.astype(jnp.int32).astype(jnp.int16)
        scales[e:e + 1, :] = lev
    dst[n * HR:n * HR + 16, :] = scales[...].astype(jnp.int32).astype(jnp.int16)


def decoder(src, n):
    lev = src[n * HR:n * HR + 16, :].astype(jnp.int32).astype(jnp.float32)
    s = jnp.exp2(lev * (1.0 / 256.0)) * (1.0 / QMAX)

    def get(e):
        q = src[e * HR:(e + 1) * HR, :].astype(jnp.int32).astype(jnp.float32)
        return q * s[e:e + 1, :]
    return get


def plus(*gets):
    return lambda e: functools.reduce(lambda p, q: p + q, [g(e) for g in gets])


def span(n):
    return pl.ds(0, n * HR + 16)


def flag(cond):
    return jnp.where(cond, 1.0, 0.0).astype(jnp.float32)


def hops():
    found = {}
    for k, off in enumerate(OFFS):
        for i in range(2):
            for u in range(2):
                sign = off if i == 0 else -off
                if sign in (0, 1, 2) or (sign == 3 and u == i):
                    found[k, i, u] = len(found)
    return found


HOPS = hops()


def kernel(seg, segv, x_any, dy_any, out, x, dy, msk, xo_h, xo_c, xh_p, xg, dyh_o, dyh_p, dyc, dyg, rel, lhs, part, hp,
           xa_s, xa_r, xb_s, xb_r, z_s, z_r, cz_s, cz_r, cr, cxa_r, cx_s, cxb_r, hz_s, hz_r, hr, ha_r, hs_s, hb_r,
           ga_s, ga_r, gb_s, gb_r, hq, hq_s, hq_r, hy, hy_s, hy_r, scales, res,
           dsem, xsem, asem, bsem, zsem, csem, cxsem, hsem, hxsem, gsem, qsem, tsem, lsem):
    dp, ex = lax.axis_index("dp"), lax.axis_index("expert")
    z, xh, c = dp // 4, (dp // 2) % 2, dp % 2
    xl, y = ex // NY, ex % NY
    X = xh * 2 + xl

    def at(z_=z, x_=X, c_=c, y_=y):
        return (z_ * 4 + (x_ // 2) * 2 + c_, (x_ % 2) * NY + y_)

    yp, ym, y2 = (y + 1) % NY, (y + 3) % NY, (y + 2) % NY
    xp, xm, x2 = (X + 1) % NX, (X + 3) % NX, (X + 2) % NX
    zp, zm = (z + 1) % NZ, (z + 7) % NZ
    partner = at(c_=1 - c)
    up, down = at(y_=yp), at(y_=ym)
    right, left = at(x_=xp), at(x_=xm)
    ahead, behind = at(z_=zp), at(z_=zm)
    g_me, g_pa = y * 2 + c, y * 2 + 1 - c

    barrier = pltpu.get_barrier_semaphore()
    for other in (partner, up, down, right, left, ahead, behind):
        pl.semaphore_signal(barrier, inc=1, device_id=other, device_id_type=pl.DeviceIdType.MESH)
    load_dy = pltpu.make_async_copy(dy_any, dy, lsem.at[0])
    load_x = pltpu.make_async_copy(x_any, x, lsem.at[1])
    load_dy.start()
    load_x.start()
    scales[...] = jnp.zeros_like(scales)

    twos = jnp.min(jnp.where(segv[...] == 2, 1.0, 0.0), axis=1, keepdims=True)
    index = lax.broadcasted_iota(jnp.int32, (NE, 1), 0)
    hot = jnp.min(jnp.where(twos > 0.5, index, NE))

    def cold_blocks(g):
        device = ((dp // 2) * 2 + g % 2) * NG + xl * NY + g // 2
        ends, first, total = [], 0, 0
        for e in range(NE):
            n = seg[e, device]
            total = total + n
            ends.append(total)
            first = first + jnp.where(e < hot, n, 0)
        picked = []
        for j in range(2):
            low = j < first
            at_ = jnp.where(low, j, j + 2)
            owner = 0
            for e in range(NE):
                owner = owner + jnp.where(ends[e] <= at_, 1, 0)
            picked.append((low, owner))
        return picked

    for g in range(NG):
        for j, (_, owner) in enumerate(cold_blocks(g)):
            for e in range(NC):
                name = e + jnp.where(e >= hot, 1, 0)
                lanes = slice((g % GG) * TOK + j * BLOCK, (g % GG) * TOK + (j + 1) * BLOCK)
                msk[g // GG, e:e + 1, lanes] = jnp.full((1, BLOCK), flag(owner == name), jnp.float32)
    low = [flag(c_[0]) for c_ in cold_blocks(g_me)]

    def pick(ref, j, i, n, width):
        w = low[j] if i == 1 else 1.0 - low[j]
        a, b = ref[j * BLOCK:(j + 1) * BLOCK, n], ref[(j + 2) * BLOCK:(j + 3) * BLOCK, n]
        return (a * jnp.full((1, width), w, jnp.float32).astype(a.dtype)
                + b * jnp.full((1, width), 1.0 - w, jnp.float32).astype(b.dtype))

    load_dy.wait()
    for i, dst in ((1, dyc), (0, dyh_o)):
        for j in range(2):
            dst[j * BLOCK:(j + 1) * BLOCK, :] = pick(dy, j, i, slice(0, 8 * FC), 8 * FC)
    load_x.wait()
    pl.semaphore_wait(barrier, 7)

    started = []

    def copy(src, dst, sem, dev):
        return pltpu.make_async_remote_copy(
            src_ref=src, dst_ref=dst, send_sem=sem.at[0], recv_sem=sem.at[1],
            device_id=dev, device_id_type=pl.DeviceIdType.MESH)

    def send(src, dst, sem, dev):
        op = copy(src, dst, sem, dev)
        op.start()
        started.append(op)

    def arrived(dst, sem):
        copy(dst, dst, sem, partner).wait_recv()

    def cols(yy, j):
        return pl.ds(pl.multiple_of((j * NY + yy) * FC, FC), FC)

    def dyslot(j, g):
        return dyg.at[j, pl.ds(pl.multiple_of(g * TOK, TOK), TOK)]

    send(dyc.at[:, cols(y2, 0)], rel.at[0], dsem.at[0], up)
    send(dyc.at[:, cols(y2, 1)], rel.at[1], dsem.at[1], down)
    send(dyh_o, dyh_p, tsem.at[0], partner)
    for j in range(2):
        send(dyc.at[:, cols(yp, j)], dyslot(j, g_me), dsem.at[2 + j], up)
        send(dyc.at[:, cols(ym, j)], dyslot(j, g_me), dsem.at[4 + j], down)
        send(dyc.at[:, cols(y, j)], dyslot(j, g_me), dsem.at[6 + j], partner)
    for j in range(2):
        dyg[j, pl.ds(pl.multiple_of(g_me * TOK, TOK), TOK)] = dyc[:, cols(y, j)]

    def turn(n, _):
        for j in range(4):
            t = pick(x, j % 2, j // 2, pl.ds(pl.multiple_of(n * BLOCK, BLOCK), BLOCK), BLOCK).T
            dst = (xo_h, xo_c)[j // 2]
            for i in range(4):
                dst[i % 2, n, i // 2, :, (j % 2) * BLOCK:(j % 2 + 1) * BLOCK] = t[i * HR:(i + 1) * HR, :]
        return 0
    lax.fori_loop(0, NZ, turn, 0)
    send(xo_h.at[1 - c], xh_p, tsem.at[1], partner)
    send(xo_c.at[1 - c], xg.at[g_me], tsem.at[2], partner)
    xg[g_me] = xo_c[c]

    def zof(k):
        return (z + OFFS[k] + NZ) % NZ

    def xsend(k):
        zk = zof(k)
        for i, (s, g) in enumerate(((xo_c.at[c, zk], g_me), (xg.at[g_pa, zk], g_pa))):
            send(s, xg.at[g, zk], xsem.at[k * 6 + i], up)
            send(s, xg.at[g, zk], xsem.at[k * 6 + 2 + i], down)

    def xforward(k):
        zk = zof(k)
        for i in range(2):
            g_d, g_u = ym * 2 + (c if i == 0 else 1 - c), yp * 2 + (c if i == 0 else 1 - c)
            arrived(xg.at[g_d, zk], xsem.at[k * 6 + i])
            arrived(xg.at[g_u, zk], xsem.at[k * 6 + 2 + i])
        send(xg.at[ym * 2 + c, zk], xg.at[ym * 2 + c, zk], xsem.at[k * 6 + 4], up)
        send(xg.at[yp * 2 + 1 - c, zk], xg.at[yp * 2 + 1 - c, zk], xsem.at[k * 6 + 5], down)

    def hmultiply():
        left_ = jnp.concatenate([xo_h[c].reshape(NZ * 2 * HR, TOK), xh_p[...].reshape(NZ * 2 * HR, TOK)], axis=1)
        for n in range(8):
            r = jnp.concatenate([dyh_o[:, n * FC:(n + 1) * FC], dyh_p[:, n * FC:(n + 1) * FC]], axis=0)
            hp[n] = jnp.dot(left_, r, preferred_element_type=jnp.float32).reshape(NZ, 2, HR, FC)

    def over_z(rows_of, n, s_, r_, sem, last):
        def step(k):
            off = OFFS[k]
            for u in range(2):
                terms = [rows_of(k, u)]
                for i in range(2):
                    if (k, i, u) in HOPS:
                        m = HOPS[k, i, u]
                        arrived(r_.at[m], sem.at[m])
                        terms.append(decoder(r_.at[m], n) if n > 1 else lambda e, m=m: r_[m])
                get = plus(*terms)
                if off == 0:
                    for e in range(n):
                        last(u, e, get(e))
                    continue
                i = u if off == 4 else (0 if off > 0 else 1)
                m = HOPS[OFFS.index((3, -3)[i] if off == 4 else (off - 1 if off > 0 else off + 1)), i, u]
                if n > 1:
                    encode(s_.at[k, u], scales, n, get)
                else:
                    s_[k, u] = get(0)
                send(s_.at[k, u], r_.at[m], sem.at[m], (ahead, behind)[i])
        return step

    def over_x(acc, a_r, s_, b_r, sem):
        way = ((0, xp, right), (1, xm, left))

        def begin():
            for i, x_, dev in way:
                send(acc.at[x2, i], a_r.at[i], sem.at[i], dev)
                send(acc.at[x_, 1 - i], b_r.at[i, 1 - i], sem.at[2 + i * 2 + 1 - i], dev)

        def middle():
            for i, x_, dev in way:
                arrived(a_r.at[i], sem.at[i])
                s_[i] = acc[x_, i] + a_r[i]
                send(s_.at[i], b_r.at[i, i], sem.at[2 + i * 2 + i], dev)

        def end(put):
            for i in range(2):
                for e in range(2):
                    arrived(b_r.at[i, e], sem.at[2 + i * 2 + e])
            for e in range(2):
                put(e, acc[X, e] + b_r[0, e] + b_r[1, e])
        return begin, middle, end

    def hrows(k, u):
        zk = zof(k)
        return lambda i: hp[(i // 2) * NY + 2 + i % 2, zk, u]

    def hput(u, i, v):
        hr[u * 2 + i // 2, i % 2] = v

    def hyput(e, v):
        hy[2 + e] = v

    hz = over_z(hrows, 4, hz_s, hz_r, hsem, hput)
    hx_begin, hx_middle, hx_end = over_x(hr, ha_r, hs_s, hb_r, hxsem)

    def grows(x_, t):
        return lambda i: hp[(x_ % 2) * NY + i % 2, 2 * t + i // 2, x_ // 2]

    def gsend(src, rcv, sem, dev, get):
        encode(src, scales, 4, get)
        send(src, rcv, sem, dev)

    def gx_begin():
        for t, dev in ((0, right), (2, left), (1, right), (3, left)):
            gsend(ga_s.at[t], ga_r.at[t], gsem.at[t], dev, grows(x2, t))
        for i, t, x_, dev in ((0, 2, xp, right), (1, 0, xm, left), (0, 3, xp, right), (1, 1, xm, left)):
            gsend(gb_s.at[i, t], gb_r.at[i, t], gsem.at[4 + i * 4 + t], dev, grows(x_, t))

    def gx_middle():
        for i, t, x_, dev in ((0, 0, xp, right), (1, 2, xm, left), (0, 1, xp, right), (1, 3, xm, left)):
            arrived(ga_r.at[t], gsem.at[t])
            gsend(gb_s.at[i, t], gb_r.at[i, t], gsem.at[4 + i * 4 + t], dev, plus(grows(x_, t), decoder(ga_r.at[t], 4)))

    def gx_end():
        for t in range(4):
            for i in range(2):
                arrived(gb_r.at[i, t], gsem.at[4 + i * 4 + t])
            get = plus(grows(X, t), decoder(gb_r.at[0, t], 4), decoder(gb_r.at[1, t], 4))
            for i in range(4):
                hq[i % 2, 2 * t + i // 2] = get(i)

    def qrows(k, u):
        zk = zof(k)
        return lambda e: hq[u, zk]

    def qput(u, e, v):
        hy[u] = v

    gz = over_z(qrows, 1, hq_s, hq_r, qsem, qput)

    def hy_begin():
        send(hy.at[y2], hy_r.at[0], tsem.at[3], up)
        send(hy.at[ym], hy_r.at[2], tsem.at[4], down)

    def hy_middle():
        arrived(hy_r.at[0], tsem.at[3])
        hy_s[...] = hy[yp] + hy_r[0]
        send(hy_s, hy_r.at[1], tsem.at[5], up)

    def hy_end():
        arrived(hy_r.at[2], tsem.at[4])
        arrived(hy_r.at[1], tsem.at[5])
        res[0] = hy[y] + hy_r[1] + hy_r[2]

    def multiply(k):
        b, zk = k, zof(k)
        for q in range(NG // GG):
            for h in range(2):
                v = jnp.concatenate([xg[q * GG + i, zk, h] for i in range(GG)], axis=1)
                for e in range(NC):
                    lhs[(h * NC + e) * HR:(h * NC + e + 1) * HR, :] = v * msk[q, e:e + 1, :].astype(v.dtype)
            for j in range(2):
                r = jnp.dot(lhs[...], dyg[j, q * GG * TOK:(q + 1) * GG * TOK, :], preferred_element_type=jnp.float32)
                r = r.reshape(2, NC * HR, FC)
                part[b, j] = r if q == 0 else part[b, j] + r

    def rows(k, x_, h):
        return lambda e: part[k, x_ % 2, x_ // 2, (h * NB[0] + e) * HR:(h * NB[0] + e + 1) * HR, :]

    def compute(k):
        multiply(k)
        for h, dev in ((0, right), (1, left)):
            encode(xa_s.at[k, h], scales, NB[h], rows(k, x2, h))
            send(xa_s.at[k, h, span(NB[h])], xa_r.at[k, h, span(NB[h])], asem.at[k * 2 + h], dev)
        for i, h, x_, dev in ((0, 1, xp, right), (1, 0, xm, left)):
            encode(xb_s.at[k, i, h], scales, NB[h], rows(k, x_, h))
            send(xb_s.at[k, i, h, span(NB[h])], xb_r.at[k, i, h, span(NB[h])], bsem.at[k * 4 + i * 2 + h], dev)

    def xsum(k):
        for h, x_, dev in ((0, xp, right), (1, xm, left)):
            arrived(xa_r.at[k, h, span(NB[h])], asem.at[k * 2 + h])
            encode(xb_s.at[k, h, h], scales, NB[h], plus(rows(k, x_, h), decoder(xa_r.at[k, h], NB[h])))
            send(xb_s.at[k, h, h, span(NB[h])], xb_r.at[k, h, h, span(NB[h])], bsem.at[k * 4 + h * 2 + h], dev)

    def zsum(k):
        off = OFFS[k]
        for h in range(2):
            n = NB[h]
            for i in range(2):
                arrived(xb_r.at[k, i, h, span(n)], bsem.at[k * 4 + i * 2 + h])
            terms = [rows(k, X, h), decoder(xb_r.at[k, 0, h], n), decoder(xb_r.at[k, 1, h], n)]
            for i in range(2):
                if (k, i, h) in HOPS:
                    m = HOPS[k, i, h]
                    arrived(z_r.at[m, span(n)], zsem.at[m])
                    terms.append(decoder(z_r.at[m], n))
            get = plus(*terms)
            if off == 0:
                for e in range(n):
                    res[1 + h * NB[0] + e] = get(e)
                continue
            encode(z_s.at[k, h], scales, n, get)
            i = h if off == 4 else (0 if off > 0 else 1)
            m = HOPS[OFFS.index((3, -3)[i] if off == 4 else (off - 1 if off > 0 else off + 1)), i, h]
            send(z_s.at[k, h, span(n)], z_r.at[m, span(n)], zsem.at[m], (ahead, behind)[i])

    def czrows(k, u):
        return lambda i: part[k, i // 2, u, (NX1 + i % 2) * HR:(NX1 + i % 2 + 1) * HR, :]

    def czput(u, i, v):
        cr[u * 2 + i // 2, i % 2] = v

    def cxput(e, v):
        res[1 + NX1 + e] = v

    czsum = over_z(czrows, 4, cz_s, cz_r, csem, czput)
    cx_begin, cx_middle, cx_end = over_x(cr, cxa_r, cx_s, cxb_r, cxsem)

    arrived(xh_p, tsem.at[1])
    arrived(dyh_p, tsem.at[0])
    hmultiply()
    gx_begin()
    hz(0)
    arrived(rel.at[0], dsem.at[0])
    send(rel.at[0], dyslot(0, ym * 2 + c), dsem.at[8], up)
    arrived(rel.at[1], dsem.at[1])
    send(rel.at[1], dyslot(1, yp * 2 + c), dsem.at[9], down)
    arrived(xg.at[g_pa], tsem.at[2])
    xsend(0)
    xsend(1)
    hz(1)
    hz(2)
    gd, gu, gf = ym * 2 + c, yp * 2 + c, y2 * 2 + c

    def relay(n, g, j, i):
        arrived(dyslot(j, g), dsem.at[i])
        send(dyslot(j, g), dyslot(j, g), dsem.at[n], partner)

    relay(10, gd, 0, 2)
    relay(11, gu, 0, 4)
    gx_middle()
    relay(12, gd, 1, 3)
    relay(13, gu, 1, 5)
    relay(14, gf, 0, 8)
    relay(15, gf, 1, 9)
    xforward(0)
    gx_end()
    gz(0)
    pd, pu, pf = ym * 2 + 1 - c, yp * 2 + 1 - c, y2 * 2 + 1 - c
    for g, j, s in ((g_pa, 0, 6), (g_pa, 1, 7), (pd, 0, 10), (pu, 0, 11), (pd, 1, 12), (pu, 1, 13), (pf, 0, 14), (pf, 1, 15)):
        arrived(dyslot(j, g), dsem.at[s])

    def chunk(k):
        if k + 2 < NZ:
            xsend(k + 2)
        if k + 1 < NZ:
            xforward(k + 1)
        zk = zof(k)
        arrived(xg.at[y2 * 2 + c, zk], xsem.at[k * 6 + 4])
        arrived(xg.at[y2 * 2 + 1 - c, zk], xsem.at[k * 6 + 5])
        compute(k)

    chunk(0)
    czsum(0)
    hz(3)
    hz(4)
    chunk(1)
    chunk(2)
    xsum(0)
    czsum(1)
    czsum(2)
    gz(1)
    gz(2)
    chunk(3)
    xsum(1)
    hz(5)
    hz(6)
    chunk(4)
    xsum(2)
    zsum(0)
    czsum(3)
    czsum(4)
    gz(3)
    gz(4)
    chunk(5)
    xsum(3)
    hz(7)
    hx_begin()
    chunk(6)
    xsum(4)
    zsum(1)
    zsum(2)
    czsum(5)
    czsum(6)
    gz(5)
    gz(6)
    chunk(7)
    xsum(5)
    hx_middle()
    xsum(6)
    zsum(3)
    zsum(4)
    gz(7)
    czsum(7)
    cx_begin()
    hx_end(hyput)
    hy_begin()
    xsum(7)
    cx_middle()
    zsum(5)
    zsum(6)
    hy_middle()
    cx_end(cxput)
    hy_end()
    zsum(7)
    for e in range(NE):
        v = res[0] * flag(e == hot)
        if e < NC:
            v = v + res[1 + e] * flag(e < hot)
        if e > 0:
            v = v + res[e] * flag(e > hot)
        out[e] = v
    for op in started:
        op.wait_send()


def shards(x_rows, dy_rows, seg_blocks):
    bf16, f32, i16 = jnp.bfloat16, jnp.float32, jnp.int16
    vm = pl.BlockSpec(memory_space=pltpu.VMEM)
    sem = pltpu.SemaphoreType.DMA
    nh = len(HOPS)
    return pl.pallas_call(
        kernel,
        out_shape=jax.ShapeDtypeStruct((NE, HR, FC), f32),
        in_specs=[pl.BlockSpec(memory_space=pltpu.SMEM), vm] + [pl.BlockSpec(memory_space=pl.ANY)] * 2,
        out_specs=vm,
        scratch_shapes=[
            pltpu.VMEM(x_rows.shape, bf16),
            pltpu.VMEM(dy_rows.shape, bf16),
            pltpu.VMEM((NG // GG, NE, GG * TOK), f32),
            pltpu.VMEM((2, NZ, 2, HR, TOK), bf16),
            pltpu.VMEM((2, NZ, 2, HR, TOK), bf16),
            pltpu.VMEM((NZ, 2, HR, TOK), bf16),
            pltpu.VMEM((NG, NZ, 2, HR, TOK), bf16),
            pltpu.VMEM((TOK, 8 * FC), bf16),
            pltpu.VMEM((TOK, 8 * FC), bf16),
            pltpu.VMEM((TOK, 8 * FC), bf16),
            pltpu.VMEM((2, NG * TOK, FC), bf16),
            pltpu.VMEM((2, TOK, FC), bf16),
            pltpu.VMEM((2 * NC * HR, GG * TOK), bf16),
            pltpu.VMEM((NZ, 2, 2, NC * HR, FC), f32),
            pltpu.VMEM((8, NZ, 2, HR, FC), f32),
            pltpu.VMEM((NZ, 2, MSG, FC), i16),
            pltpu.VMEM((NZ, 2, MSG, FC), i16),
            pltpu.VMEM((NZ, 2, 2, MSG, FC), i16),
            pltpu.VMEM((NZ, 2, 2, MSG, FC), i16),
            pltpu.VMEM((NZ, 2, MSG, FC), i16),
            pltpu.VMEM((nh, MSG, FC), i16),
            pltpu.VMEM((NZ, 2, MSG, FC), i16),
            pltpu.VMEM((nh, MSG, FC), i16),
            pltpu.VMEM((4, 2, HR, FC), f32),
            pltpu.VMEM((2, HR, FC), f32),
            pltpu.VMEM((2, HR, FC), f32),
            pltpu.VMEM((2, 2, HR, FC), f32),
            pltpu.VMEM((NZ, 2, MSG, FC), i16),
            pltpu.VMEM((nh, MSG, FC), i16),
            pltpu.VMEM((4, 2, HR, FC), f32),
            pltpu.VMEM((2, HR, FC), f32),
            pltpu.VMEM((2, HR, FC), f32),
            pltpu.VMEM((2, 2, HR, FC), f32),
            pltpu.VMEM((4, MSG, FC), i16),
            pltpu.VMEM((4, MSG, FC), i16),
            pltpu.VMEM((2, 4, MSG, FC), i16),
            pltpu.VMEM((2, 4, MSG, FC), i16),
            pltpu.VMEM((2, NZ, HR, FC), f32),
            pltpu.VMEM((NZ, 2, HR, FC), f32),
            pltpu.VMEM((nh, HR, FC), f32),
            pltpu.VMEM((4, HR, FC), f32),
            pltpu.VMEM((HR, FC), f32),
            pltpu.VMEM((3, HR, FC), f32),
            pltpu.VMEM((16, FC), f32),
            pltpu.VMEM((NE, HR, FC), f32),
            sem((16, 2)), sem((48, 2)), sem((16, 2)), sem((32, 2)), sem((nh, 2)), sem((nh, 2)), sem((6, 2)),
            sem((nh, 2)), sem((6, 2)), sem((12, 2)), sem((nh, 2)), sem((6, 2)), sem((2,)),
        ],
        compiler_params=pltpu.CompilerParams(
            collective_id=0, has_side_effects=True, vmem_limit_bytes=58 << 20),
    )(seg_blocks.T, seg_blocks.T, x_rows, dy_rows)


def solution(mesh):
    in_specs = (P(("dp", "expert"), None), P(("dp", "expert"), None), P())
    out_specs = P(None, "dp", "expert")
    return jax.shard_map(shards, mesh=mesh, in_specs=in_specs, out_specs=out_specs, check_vma=False)
```

```python
import functools

import jax
import jax.numpy as jnp
from jax import lax
from jax.experimental import pallas as pl
from jax.experimental.pallas import tpu as pltpu
from jax.sharding import PartitionSpec as P

BLOCK = 128
NE = 8
NC = NE - 1
NX1 = 5
NB = (3, 2)
TOK = 2 * BLOCK
NY, NX, NZ = 4, 4, 8
NG = 2 * NY
GG = 4
HR, FC = 32, 256
MSG = 4 * HR + 16
OFFS = (4, 3, -3, 2, -2, 1, -1, 0)
QMAX = 32700.0


def encode(dst, scales, n, get):
    for e in range(n):
        v = get(e)
        top = jnp.max(jnp.abs(v), axis=0, keepdims=True)
        lev = jnp.ceil(jnp.log2(jnp.maximum(top, 1e-30)) * 256.0) + 1.0
        q = jnp.round(v * (jnp.exp2(lev * (-1.0 / 256.0)) * QMAX))
        dst[e * HR:(e + 1) * HR, :] = q.astype(jnp.int32).astype(jnp.int16)
        scales[e:e + 1, :] = lev
    dst[n * HR:n * HR + 16, :] = scales[...].astype(jnp.int32).astype(jnp.int16)


def decoder(src, n):
    lev = src[n * HR:n * HR + 16, :].astype(jnp.int32).astype(jnp.float32)
    s = jnp.exp2(lev * (1.0 / 256.0)) * (1.0 / QMAX)

    def get(e):
        q = src[e * HR:(e + 1) * HR, :].astype(jnp.int32).astype(jnp.float32)
        return q * s[e:e + 1, :]
    return get


def plus(*gets):
    return lambda e: functools.reduce(lambda p, q: p + q, [g(e) for g in gets])


def span(n):
    return pl.ds(0, n * HR + 16)


def flag(cond):
    return jnp.where(cond, 1.0, 0.0).astype(jnp.float32)


def hops():
    found = {}
    for k, off in enumerate(OFFS):
        for i in range(2):
            for u in range(2):
                sign = off if i == 0 else -off
                if sign in (0, 1, 2) or (sign == 3 and u == i):
                    found[k, i, u] = len(found)
    return found


HOPS = hops()


def kernel(seg, segv, x_any, dy_any, out, x, dy, msk, xo_h, xo_c, xh_p, xg, dyh_o, dyh_p, dyc, dyg, rel, lhs, part, hp,
           xa_s, xa_r, xb_s, xb_r, z_s, z_r, cz_s, cz_r, cr, cxa_r, cx_s, cxb_r, hz_s, hz_r, hr, ha_r, hs_s, hb_r,
           ga_s, ga_r, gb_s, gb_r, hq, hq_s, hq_r, hy, hy_s, hy_r, scales, res,
           dsem, xsem, asem, bsem, zsem, csem, cxsem, hsem, hxsem, gsem, qsem, tsem, lsem, ssem):
    dp, ex = lax.axis_index("dp"), lax.axis_index("expert")
    z, xh, c = dp // 4, (dp // 2) % 2, dp % 2
    xl, y = ex // NY, ex % NY
    X = xh * 2 + xl

    def at(z_=z, x_=X, c_=c, y_=y):
        return (z_ * 4 + (x_ // 2) * 2 + c_, (x_ % 2) * NY + y_)

    yp, ym, y2 = (y + 1) % NY, (y + 3) % NY, (y + 2) % NY
    xp, xm, x2 = (X + 1) % NX, (X + 3) % NX, (X + 2) % NX
    zp, zm = (z + 1) % NZ, (z + 7) % NZ
    partner = at(c_=1 - c)
    up, down = at(y_=yp), at(y_=ym)
    right, left = at(x_=xp), at(x_=xm)
    ahead, behind = at(z_=zp), at(z_=zm)
    g_me, g_pa = y * 2 + c, y * 2 + 1 - c

    barrier = pltpu.get_barrier_semaphore()
    for other in (partner, up, down, right, left, ahead, behind):
        pl.semaphore_signal(barrier, inc=1, device_id=other, device_id_type=pl.DeviceIdType.MESH)
    load_dy = pltpu.make_async_copy(dy_any, dy, lsem.at[0])
    load_x = pltpu.make_async_copy(x_any, x, lsem.at[1])
    load_dy.start()
    load_x.start()
    scales[...] = jnp.zeros_like(scales)

    twos = jnp.min(jnp.where(segv[...] == 2, 1.0, 0.0), axis=1, keepdims=True)
    index = lax.broadcasted_iota(jnp.int32, (NE, 1), 0)
    hot = jnp.min(jnp.where(twos > 0.5, index, NE))

    def cold_blocks(g):
        device = ((dp // 2) * 2 + g % 2) * NG + xl * NY + g // 2
        ends, first, total = [], 0, 0
        for e in range(NE):
            n = seg[e, device]
            total = total + n
            ends.append(total)
            first = first + jnp.where(e < hot, n, 0)
        picked = []
        for j in range(2):
            low = j < first
            at_ = jnp.where(low, j, j + 2)
            owner = 0
            for e in range(NE):
                owner = owner + jnp.where(ends[e] <= at_, 1, 0)
            picked.append((low, owner))
        return picked

    low = [flag(c_[0]) for c_ in cold_blocks(g_me)]

    def pick(ref, j, i, n, width):
        w = low[j] if i == 1 else 1.0 - low[j]
        a, b = ref[j * BLOCK:(j + 1) * BLOCK, n], ref[(j + 2) * BLOCK:(j + 3) * BLOCK, n]
        return (a * jnp.full((1, width), w, jnp.float32).astype(a.dtype)
                + b * jnp.full((1, width), 1.0 - w, jnp.float32).astype(b.dtype))

    def choose(i, dst):
        for j in range(2):
            dst[j * BLOCK:(j + 1) * BLOCK, :] = pick(dy, j, i, slice(0, 8 * FC), 8 * FC)

    load_dy.wait()
    choose(1, dyc)
    pl.semaphore_wait(barrier, 7)

    started = []

    def copy(src, dst, sem, dev):
        return pltpu.make_async_remote_copy(
            src_ref=src, dst_ref=dst, send_sem=ssem.at[0], recv_sem=sem,
            device_id=dev, device_id_type=pl.DeviceIdType.MESH)

    def send(src, dst, sem, dev):
        op = copy(src, dst, sem, dev)
        op.start()
        started.append(op)

    def arrived(dst, sem):
        copy(dst, dst, sem, partner).wait_recv()

    def cols(yy, j):
        return pl.ds(pl.multiple_of((j * NY + yy) * FC, FC), FC)

    def dyslot(j, g):
        return dyg.at[j, pl.ds(pl.multiple_of(g * TOK, TOK), TOK)]

    send(dyc.at[:, cols(y2, 0)], rel.at[0], dsem.at[0], up)
    send(dyc.at[:, cols(y2, 1)], rel.at[1], dsem.at[1], down)
    for j in range(2):
        send(dyc.at[:, cols(yp, j)], dyslot(j, g_me), dsem.at[2 + j], up)
        send(dyc.at[:, cols(ym, j)], dyslot(j, g_me), dsem.at[4 + j], down)
        send(dyc.at[:, cols(y, j)], dyslot(j, g_me), dsem.at[6 + j], partner)
    choose(0, dyh_o)
    send(dyh_o, dyh_p, tsem.at[0], partner)
    for j in range(2):
        dyg[j, pl.ds(pl.multiple_of(g_me * TOK, TOK), TOK)] = dyc[:, cols(y, j)]
    load_x.wait()

    def turn(n, _):
        for j in range(4):
            t = pick(x, j % 2, j // 2, pl.ds(pl.multiple_of(n * BLOCK, BLOCK), BLOCK), BLOCK).T
            dst = (xo_h, xo_c)[j // 2]
            for i in range(4):
                dst[i % 2, n, i // 2, :, (j % 2) * BLOCK:(j % 2 + 1) * BLOCK] = t[i * HR:(i + 1) * HR, :]
        return 0
    lax.fori_loop(0, NZ, turn, 0)
    send(xo_h.at[1 - c], xh_p, tsem.at[1], partner)
    send(xo_c.at[1 - c], xg.at[g_me], tsem.at[2], partner)
    xg[g_me] = xo_c[c]

    def zof(k):
        return (z + OFFS[k] + NZ) % NZ

    def xsend(k):
        zk = zof(k)
        for i, (s, g) in enumerate(((xo_c.at[c, zk], g_me), (xg.at[g_pa, zk], g_pa))):
            send(s, xg.at[g, zk], xsem.at[k * 6 + i], up)
            send(s, xg.at[g, zk], xsem.at[k * 6 + 2 + i], down)

    def xforward(k):
        zk = zof(k)
        for i in range(2):
            g_d, g_u = ym * 2 + (c if i == 0 else 1 - c), yp * 2 + (c if i == 0 else 1 - c)
            arrived(xg.at[g_d, zk], xsem.at[k * 6 + i])
            arrived(xg.at[g_u, zk], xsem.at[k * 6 + 2 + i])
        send(xg.at[ym * 2 + c, zk], xg.at[ym * 2 + c, zk], xsem.at[k * 6 + 4], up)
        send(xg.at[yp * 2 + 1 - c, zk], xg.at[yp * 2 + 1 - c, zk], xsem.at[k * 6 + 5], down)

    def hmultiply():
        left_ = jnp.concatenate([xo_h[c].reshape(NZ * 2 * HR, TOK), xh_p[...].reshape(NZ * 2 * HR, TOK)], axis=1)
        for n in range(8):
            r = jnp.concatenate([dyh_o[:, n * FC:(n + 1) * FC], dyh_p[:, n * FC:(n + 1) * FC]], axis=0)
            hp[n] = jnp.dot(left_, r, preferred_element_type=jnp.float32).reshape(NZ, 2, HR, FC)

    def over_z(rows_of, n, s_, r_, sem, last):
        def step(k):
            off = OFFS[k]
            for u in range(2):
                terms = [rows_of(k, u)]
                for i in range(2):
                    if (k, i, u) in HOPS:
                        m = HOPS[k, i, u]
                        arrived(r_.at[m], sem.at[m])
                        terms.append(decoder(r_.at[m], n) if n > 1 else lambda e, m=m: r_[m])
                get = plus(*terms)
                if off == 0:
                    for e in range(n):
                        last(u, e, get(e))
                    continue
                i = u if off == 4 else (0 if off > 0 else 1)
                m = HOPS[OFFS.index((3, -3)[i] if off == 4 else (off - 1 if off > 0 else off + 1)), i, u]
                if n > 1:
                    encode(s_.at[k, u], scales, n, get)
                else:
                    s_[k, u] = get(0)
                send(s_.at[k, u], r_.at[m], sem.at[m], (ahead, behind)[i])
        return step

    def over_x(acc, a_r, s_, b_r, sem):
        way = ((0, xp, right), (1, xm, left))

        def begin():
            for i, x_, dev in way:
                send(acc.at[x2, i], a_r.at[i], sem.at[i], dev)
                send(acc.at[x_, 1 - i], b_r.at[i, 1 - i], sem.at[2 + i * 2 + 1 - i], dev)

        def middle():
            for i, x_, dev in way:
                arrived(a_r.at[i], sem.at[i])
                s_[i] = acc[x_, i] + a_r[i]
                send(s_.at[i], b_r.at[i, i], sem.at[2 + i * 2 + i], dev)

        def end(put):
            for i in range(2):
                for e in range(2):
                    arrived(b_r.at[i, e], sem.at[2 + i * 2 + e])
            for e in range(2):
                put(e, acc[X, e] + b_r[0, e] + b_r[1, e])
        return begin, middle, end

    def hrows(k, u):
        zk = zof(k)
        return lambda i: hp[(i // 2) * NY + 2 + i % 2, zk, u]

    def hput(u, i, v):
        hr[u * 2 + i // 2, i % 2] = v

    def hyput(e, v):
        hy[2 + e] = v

    hz = over_z(hrows, 4, hz_s, hz_r, hsem, hput)
    hx_begin, hx_middle, hx_end = over_x(hr, ha_r, hs_s, hb_r, hxsem)

    def grows(x_, t):
        return lambda i: hp[(x_ % 2) * NY + i % 2, 2 * t + i // 2, x_ // 2]

    def gsend(src, rcv, sem, dev, get):
        encode(src, scales, 4, get)
        send(src, rcv, sem, dev)

    def gx_begin():
        for t, dev in ((0, right), (2, left), (1, right), (3, left)):
            gsend(ga_s.at[t], ga_r.at[t], gsem.at[t], dev, grows(x2, t))
        for i, t, x_, dev in ((0, 2, xp, right), (1, 0, xm, left), (0, 3, xp, right), (1, 1, xm, left)):
            gsend(gb_s.at[i, t], gb_r.at[i, t], gsem.at[4 + i * 4 + t], dev, grows(x_, t))

    def gx_middle():
        for i, t, x_, dev in ((0, 0, xp, right), (1, 2, xm, left), (0, 1, xp, right), (1, 3, xm, left)):
            arrived(ga_r.at[t], gsem.at[t])
            gsend(gb_s.at[i, t], gb_r.at[i, t], gsem.at[4 + i * 4 + t], dev, plus(grows(x_, t), decoder(ga_r.at[t], 4)))

    def gx_end():
        for t in range(4):
            for i in range(2):
                arrived(gb_r.at[i, t], gsem.at[4 + i * 4 + t])
            get = plus(grows(X, t), decoder(gb_r.at[0, t], 4), decoder(gb_r.at[1, t], 4))
            for i in range(4):
                hq[i % 2, 2 * t + i // 2] = get(i)

    def qrows(k, u):
        zk = zof(k)
        return lambda e: hq[u, zk]

    def qput(u, e, v):
        hy[u] = v

    gz = over_z(qrows, 1, hq_s, hq_r, qsem, qput)

    def hy_begin():
        send(hy.at[y2], hy_r.at[0], tsem.at[3], up)
        send(hy.at[ym], hy_r.at[2], tsem.at[4], down)

    def hy_middle():
        arrived(hy_r.at[0], tsem.at[3])
        hy_s[...] = hy[yp] + hy_r[0]
        send(hy_s, hy_r.at[1], tsem.at[5], up)

    def hy_end():
        arrived(hy_r.at[2], tsem.at[4])
        arrived(hy_r.at[1], tsem.at[5])
        res[0] = hy[y] + hy_r[1] + hy_r[2]

    def multiply(k):
        b, zk = k, zof(k)
        for q in range(NG // GG):
            for h in range(2):
                v = jnp.concatenate([xg[q * GG + i, zk, h] for i in range(GG)], axis=1)
                for e in range(NC):
                    lhs[(h * NC + e) * HR:(h * NC + e + 1) * HR, :] = v * msk[q, e:e + 1, :].astype(v.dtype)
            for j in range(2):
                r = jnp.dot(lhs[...], dyg[j, q * GG * TOK:(q + 1) * GG * TOK, :], preferred_element_type=jnp.float32)
                r = r.reshape(2, NC * HR, FC)
                part[b, j] = r if q == 0 else part[b, j] + r

    def rows(k, x_, h):
        return lambda e: part[k, x_ % 2, x_ // 2, (h * NB[0] + e) * HR:(h * NB[0] + e + 1) * HR, :]

    def compute(k):
        multiply(k)
        for h, dev in ((0, right), (1, left)):
            encode(xa_s.at[k, h], scales, NB[h], rows(k, x2, h))
            send(xa_s.at[k, h, span(NB[h])], xa_r.at[k, h, span(NB[h])], asem.at[k * 2 + h], dev)
        for i, h, x_, dev in ((0, 1, xp, right), (1, 0, xm, left)):
            encode(xb_s.at[k, i, h], scales, NB[h], rows(k, x_, h))
            send(xb_s.at[k, i, h, span(NB[h])], xb_r.at[k, i, h, span(NB[h])], bsem.at[k * 4 + i * 2 + h], dev)

    def xsum(k):
        for h, x_, dev in ((0, xp, right), (1, xm, left)):
            arrived(xa_r.at[k, h, span(NB[h])], asem.at[k * 2 + h])
            encode(xb_s.at[k, h, h], scales, NB[h], plus(rows(k, x_, h), decoder(xa_r.at[k, h], NB[h])))
            send(xb_s.at[k, h, h, span(NB[h])], xb_r.at[k, h, h, span(NB[h])], bsem.at[k * 4 + h * 2 + h], dev)

    def zsum(k):
        off = OFFS[k]
        for h in range(2):
            n = NB[h]
            for i in range(2):
                arrived(xb_r.at[k, i, h, span(n)], bsem.at[k * 4 + i * 2 + h])
            terms = [rows(k, X, h), decoder(xb_r.at[k, 0, h], n), decoder(xb_r.at[k, 1, h], n)]
            for i in range(2):
                if (k, i, h) in HOPS:
                    m = HOPS[k, i, h]
                    arrived(z_r.at[m, span(n)], zsem.at[m])
                    terms.append(decoder(z_r.at[m], n))
            get = plus(*terms)
            if off == 0:
                for e in range(n):
                    res[1 + h * NB[0] + e] = get(e)
                continue
            encode(z_s.at[k, h], scales, n, get)
            i = h if off == 4 else (0 if off > 0 else 1)
            m = HOPS[OFFS.index((3, -3)[i] if off == 4 else (off - 1 if off > 0 else off + 1)), i, h]
            send(z_s.at[k, h, span(n)], z_r.at[m, span(n)], zsem.at[m], (ahead, behind)[i])

    def czrows(k, u):
        return lambda i: part[k, i // 2, u, (NX1 + i % 2) * HR:(NX1 + i % 2 + 1) * HR, :]

    def czput(u, i, v):
        cr[u * 2 + i // 2, i % 2] = v

    def cxput(e, v):
        res[1 + NX1 + e] = v

    czsum = over_z(czrows, 4, cz_s, cz_r, csem, czput)
    cx_begin, cx_middle, cx_end = over_x(cr, cxa_r, cx_s, cxb_r, cxsem)

    arrived(xh_p, tsem.at[1])
    arrived(dyh_p, tsem.at[0])
    hmultiply()
    gx_begin()
    hz(0)
    for g in range(NG):
        for j, (_, owner) in enumerate(cold_blocks(g)):
            for e in range(NC):
                name = e + jnp.where(e >= hot, 1, 0)
                lanes = slice((g % GG) * TOK + j * BLOCK, (g % GG) * TOK + (j + 1) * BLOCK)
                msk[g // GG, e:e + 1, lanes] = jnp.full((1, BLOCK), flag(owner == name), jnp.float32)
    arrived(rel.at[0], dsem.at[0])
    send(rel.at[0], dyslot(0, ym * 2 + c), dsem.at[8], up)
    arrived(rel.at[1], dsem.at[1])
    send(rel.at[1], dyslot(1, yp * 2 + c), dsem.at[9], down)
    arrived(xg.at[g_pa], tsem.at[2])
    xsend(0)
    xsend(1)
    xsend(2)
    hz(1)
    hz(2)
    gd, gu, gf = ym * 2 + c, yp * 2 + c, y2 * 2 + c

    def relay(n, g, j, i):
        arrived(dyslot(j, g), dsem.at[i])
        send(dyslot(j, g), dyslot(j, g), dsem.at[n], partner)

    relay(10, gd, 0, 2)
    relay(11, gu, 0, 4)
    gx_middle()
    relay(12, gd, 1, 3)
    relay(13, gu, 1, 5)
    relay(14, gf, 0, 8)
    relay(15, gf, 1, 9)
    xforward(0)
    gx_end()
    gz(0)
    pd, pu, pf = ym * 2 + 1 - c, yp * 2 + 1 - c, y2 * 2 + 1 - c
    for g, j, s in ((g_pa, 0, 6), (g_pa, 1, 7), (pd, 0, 10), (pu, 0, 11), (pd, 1, 12), (pu, 1, 13), (pf, 0, 14), (pf, 1, 15)):
        arrived(dyslot(j, g), dsem.at[s])

    def chunk(k):
        zk = zof(k)
        arrived(xg.at[y2 * 2 + c, zk], xsem.at[k * 6 + 4])
        arrived(xg.at[y2 * 2 + 1 - c, zk], xsem.at[k * 6 + 5])
        compute(k)
        if k + 3 < NZ:
            xsend(k + 3)
        if k + 2 < NZ:
            xforward(k + 2)

    xforward(1)
    chunk(0)
    czsum(0)
    hz(3)
    hz(4)
    chunk(1)
    gz(1)
    gz(2)
    chunk(2)
    xsum(0)
    czsum(1)
    czsum(2)
    hz(5)
    hz(6)
    chunk(3)
    xsum(1)
    gz(3)
    gz(4)
    chunk(4)
    xsum(2)
    zsum(0)
    czsum(3)
    czsum(4)
    hz(7)
    hx_begin()
    chunk(5)
    xsum(3)
    gz(5)
    gz(6)
    chunk(6)
    xsum(4)
    zsum(1)
    zsum(2)
    hx_middle()
    czsum(5)
    czsum(6)
    chunk(7)
    xsum(5)
    xsum(6)
    gz(7)
    zsum(3)
    zsum(4)
    czsum(7)
    cx_begin()
    hx_end(hyput)
    hy_begin()
    xsum(7)
    cx_middle()
    zsum(5)
    zsum(6)
    hy_middle()
    cx_end(cxput)
    hy_end()
    zsum(7)
    for e in range(NE):
        v = res[0] * flag(e == hot)
        if e < NC:
            v = v + res[1 + e] * flag(e < hot)
        if e > 0:
            v = v + res[e] * flag(e > hot)
        out[e] = v
    for op in started:
        op.wait_send()


def shards(x_rows, dy_rows, seg_blocks):
    bf16, f32, i16 = jnp.bfloat16, jnp.float32, jnp.int16
    vm = pl.BlockSpec(memory_space=pltpu.VMEM)
    sem = pltpu.SemaphoreType.DMA
    nh = len(HOPS)
    return pl.pallas_call(
        kernel,
        out_shape=pltpu.VMEM((NE, HR, FC), f32),
        in_specs=[pl.BlockSpec(memory_space=pltpu.SMEM), vm] + [pl.BlockSpec(memory_space=pl.ANY)] * 2,
        out_specs=vm,
        scratch_shapes=[
            pltpu.VMEM(x_rows.shape, bf16),
            pltpu.VMEM(dy_rows.shape, bf16),
            pltpu.VMEM((NG // GG, NE, GG * TOK), f32),
            pltpu.VMEM((2, NZ, 2, HR, TOK), bf16),
            pltpu.VMEM((2, NZ, 2, HR, TOK), bf16),
            pltpu.VMEM((NZ, 2, HR, TOK), bf16),
            pltpu.VMEM((NG, NZ, 2, HR, TOK), bf16),
            pltpu.VMEM((TOK, 8 * FC), bf16),
            pltpu.VMEM((TOK, 8 * FC), bf16),
            pltpu.VMEM((TOK, 8 * FC), bf16),
            pltpu.VMEM((2, NG * TOK, FC), bf16),
            pltpu.VMEM((2, TOK, FC), bf16),
            pltpu.VMEM((2 * NC * HR, GG * TOK), bf16),
            pltpu.VMEM((NZ, 2, 2, NC * HR, FC), f32),
            pltpu.VMEM((8, NZ, 2, HR, FC), f32),
            pltpu.VMEM((NZ, 2, MSG, FC), i16),
            pltpu.VMEM((NZ, 2, MSG, FC), i16),
            pltpu.VMEM((NZ, 2, 2, MSG, FC), i16),
            pltpu.VMEM((NZ, 2, 2, MSG, FC), i16),
            pltpu.VMEM((NZ, 2, MSG, FC), i16),
            pltpu.VMEM((nh, MSG, FC), i16),
            pltpu.VMEM((NZ, 2, MSG, FC), i16),
            pltpu.VMEM((nh, MSG, FC), i16),
            pltpu.VMEM((4, 2, HR, FC), f32),
            pltpu.VMEM((2, HR, FC), f32),
            pltpu.VMEM((2, HR, FC), f32),
            pltpu.VMEM((2, 2, HR, FC), f32),
            pltpu.VMEM((NZ, 2, MSG, FC), i16),
            pltpu.VMEM((nh, MSG, FC), i16),
            pltpu.VMEM((4, 2, HR, FC), f32),
            pltpu.VMEM((2, HR, FC), f32),
            pltpu.VMEM((2, HR, FC), f32),
            pltpu.VMEM((2, 2, HR, FC), f32),
            pltpu.VMEM((4, MSG, FC), i16),
            pltpu.VMEM((4, MSG, FC), i16),
            pltpu.VMEM((2, 4, MSG, FC), i16),
            pltpu.VMEM((2, 4, MSG, FC), i16),
            pltpu.VMEM((2, NZ, HR, FC), f32),
            pltpu.VMEM((NZ, 2, HR, FC), f32),
            pltpu.VMEM((nh, HR, FC), f32),
            pltpu.VMEM((4, HR, FC), f32),
            pltpu.VMEM((HR, FC), f32),
            pltpu.VMEM((3, HR, FC), f32),
            pltpu.VMEM((16, FC), f32),
            pltpu.VMEM((NE, HR, FC), f32),
            sem((16,)), sem((48,)), sem((16,)), sem((32,)), sem((nh,)), sem((nh,)), sem((6,)),
            sem((nh,)), sem((6,)), sem((12,)), sem((nh,)), sem((6,)), sem((2,)), sem((1,)),
        ],
        compiler_params=pltpu.CompilerParams(
            collective_id=0, has_side_effects=True, vmem_limit_bytes=58 << 20),
    )(seg_blocks.T, seg_blocks.T, x_rows, dy_rows)


def solution(mesh):
    in_specs = (P(("dp", "expert"), None), P(("dp", "expert"), None), P())
    out_specs = P(None, "dp", "expert")
    return jax.shard_map(shards, mesh=mesh, in_specs=in_specs, out_specs=out_specs, check_vma=False)
```

```python
import functools

import jax
import jax.numpy as jnp
from jax import lax
from jax.experimental import pallas as pl
from jax.experimental.pallas import tpu as pltpu
from jax.sharding import PartitionSpec as P

BLOCK = 128
NE = 8
NC = NE - 1
NX1 = 5
NB = (3, 2)
TOK = 2 * BLOCK
NY, NX, NZ = 4, 4, 8
NG = 2 * NY
GG = 4
HR, FC = 32, 256
MSG = 4 * HR + 16
OFFS = (4, 3, -3, 2, -2, 1, -1, 0)
QMAX = 32700.0


def encode(dst, scales, n, get):
    for e in range(n):
        v = get(e)
        top = jnp.max(jnp.abs(v), axis=0, keepdims=True)
        lev = jnp.ceil(jnp.log2(jnp.maximum(top, 1e-30)) * 256.0) + 1.0
        q = jnp.round(v * (jnp.exp2(lev * (-1.0 / 256.0)) * QMAX))
        dst[e * HR:(e + 1) * HR, :] = q.astype(jnp.int32).astype(jnp.int16)
        scales[e:e + 1, :] = lev
    dst[n * HR:n * HR + 16, :] = scales[...].astype(jnp.int32).astype(jnp.int16)


def decoder(src, n):
    lev = src[n * HR:n * HR + 16, :].astype(jnp.int32).astype(jnp.float32)
    s = jnp.exp2(lev * (1.0 / 256.0)) * (1.0 / QMAX)

    def get(e):
        q = src[e * HR:(e + 1) * HR, :].astype(jnp.int32).astype(jnp.float32)
        return q * s[e:e + 1, :]
    return get


def plus(*gets):
    return lambda e: functools.reduce(lambda p, q: p + q, [g(e) for g in gets])


def span(n):
    return pl.ds(0, n * HR + 16)


def flag(cond):
    return jnp.where(cond, 1.0, 0.0).astype(jnp.float32)


def hops():
    found = {}
    for k, off in enumerate(OFFS):
        for i in range(2):
            for u in range(2):
                sign = off if i == 0 else -off
                if sign in (0, 1, 2) or (sign == 3 and u == i):
                    found[k, i, u] = len(found)
    return found


HOPS = hops()


def kernel(seg_any, x_any, dy_any, out, seg, segv, x, dy, msk, xo_h, xo_c, xh_p, xg, dyh_o, dyh_p, dyc, dyg, rel, lhs, part, hp,
           xa_s, xa_r, xb_s, xb_r, z_s, z_r, cz_s, cz_r, cr, cxa_r, cx_s, cxb_r, hz_s, hz_r, hr, ha_r, hs_s, hb_r,
           ga_s, ga_r, gb_s, gb_r, hq, hq_s, hq_r, hy, hy_s, hy_r, scales, res,
           dsem, xsem, asem, bsem, zsem, csem, cxsem, hsem, hxsem, gsem, qsem, tsem, lsem, ssem):
    dp, ex = lax.axis_index("dp"), lax.axis_index("expert")
    z, xh, c = dp // 4, (dp // 2) % 2, dp % 2
    xl, y = ex // NY, ex % NY
    X = xh * 2 + xl

    def at(z_=z, x_=X, c_=c, y_=y):
        return (z_ * 4 + (x_ // 2) * 2 + c_, (x_ % 2) * NY + y_)

    yp, ym, y2 = (y + 1) % NY, (y + 3) % NY, (y + 2) % NY
    xp, xm, x2 = (X + 1) % NX, (X + 3) % NX, (X + 2) % NX
    zp, zm = (z + 1) % NZ, (z + 7) % NZ
    partner = at(c_=1 - c)
    up, down = at(y_=yp), at(y_=ym)
    right, left = at(x_=xp), at(x_=xm)
    ahead, behind = at(z_=zp), at(z_=zm)
    g_me, g_pa = y * 2 + c, y * 2 + 1 - c

    barrier = pltpu.get_barrier_semaphore()
    for other in (partner, up, down, right, left, ahead, behind):
        pl.semaphore_signal(barrier, inc=1, device_id=other, device_id_type=pl.DeviceIdType.MESH)
    load_dy = pltpu.make_async_copy(dy_any, dy, lsem.at[0])
    load_x = pltpu.make_async_copy(x_any, x, lsem.at[1])
    loads = [pltpu.make_async_copy(seg_any, ref, lsem.at[2 + i]) for i, ref in enumerate((seg, segv))]
    for op in loads:
        op.start()
    load_dy.start()
    load_x.start()
    scales[...] = jnp.zeros_like(scales)

    for op in loads:
        op.wait()

    twos = jnp.min(jnp.where(segv[...] == 2, 1.0, 0.0), axis=1, keepdims=True)
    index = lax.broadcasted_iota(jnp.int32, (NE, 1), 0)
    hot = jnp.min(jnp.where(twos > 0.5, index, NE))

    def cold_blocks(g):
        device = ((dp // 2) * 2 + g % 2) * NG + xl * NY + g // 2
        ends, first, total = [], 0, 0
        for e in range(NE):
            n = seg[e, device]
            total = total + n
            ends.append(total)
            first = first + jnp.where(e < hot, n, 0)
        picked = []
        for j in range(2):
            low = j < first
            at_ = jnp.where(low, j, j + 2)
            owner = 0
            for e in range(NE):
                owner = owner + jnp.where(ends[e] <= at_, 1, 0)
            picked.append((low, owner))
        return picked

    low = [flag(c_[0]) for c_ in cold_blocks(g_me)]

    def pick(ref, j, i, n, width):
        w = low[j] if i == 1 else 1.0 - low[j]
        a, b = ref[j * BLOCK:(j + 1) * BLOCK, n], ref[(j + 2) * BLOCK:(j + 3) * BLOCK, n]
        return (a * jnp.full((1, width), w, jnp.float32).astype(a.dtype)
                + b * jnp.full((1, width), 1.0 - w, jnp.float32).astype(b.dtype))

    def choose(i, dst):
        for j in range(2):
            dst[j * BLOCK:(j + 1) * BLOCK, :] = pick(dy, j, i, slice(0, 8 * FC), 8 * FC)

    load_dy.wait()
    choose(1, dyc)
    pl.semaphore_wait(barrier, 7)

    started = []

    def copy(src, dst, sem, dev):
        return pltpu.make_async_remote_copy(
            src_ref=src, dst_ref=dst, send_sem=ssem.at[0], recv_sem=sem,
            device_id=dev, device_id_type=pl.DeviceIdType.MESH)

    def send(src, dst, sem, dev):
        op = copy(src, dst, sem, dev)
        op.start()
        started.append(op)

    def arrived(dst, sem):
        copy(dst, dst, sem, partner).wait_recv()

    def cols(yy, j):
        return pl.ds(pl.multiple_of((j * NY + yy) * FC, FC), FC)

    def dyslot(j, g):
        return dyg.at[j, pl.ds(pl.multiple_of(g * TOK, TOK), TOK)]

    send(dyc.at[:, cols(y2, 0)], rel.at[0], dsem.at[0], up)
    send(dyc.at[:, cols(y2, 1)], rel.at[1], dsem.at[1], down)
    for j in range(2):
        send(dyc.at[:, cols(yp, j)], dyslot(j, g_me), dsem.at[2 + j], up)
        send(dyc.at[:, cols(ym, j)], dyslot(j, g_me), dsem.at[4 + j], down)
        send(dyc.at[:, cols(y, j)], dyslot(j, g_me), dsem.at[6], partner)
    choose(0, dyh_o)
    send(dyh_o, dyh_p, tsem.at[0], partner)
    for j in range(2):
        dyg[j, pl.ds(pl.multiple_of(g_me * TOK, TOK), TOK)] = dyc[:, cols(y, j)]
    load_x.wait()

    def turn(n, _):
        for j in range(4):
            t = pick(x, j % 2, j // 2, pl.ds(pl.multiple_of(n * BLOCK, BLOCK), BLOCK), BLOCK).T
            dst = (xo_h, xo_c)[j // 2]
            for i in range(4):
                dst[i % 2, n, i // 2, :, (j % 2) * BLOCK:(j % 2 + 1) * BLOCK] = t[i * HR:(i + 1) * HR, :]
        return 0
    lax.fori_loop(0, NZ, turn, 0)
    send(xo_h.at[1 - c], xh_p, tsem.at[1], partner)
    send(xo_c.at[1 - c], xg.at[g_me], tsem.at[2], partner)
    xg[g_me] = xo_c[c]

    def zof(k):
        return (z + OFFS[k] + NZ) % NZ

    def xsend(k):
        zk = zof(k)
        for i, (s, g) in enumerate(((xo_c.at[c, zk], g_me), (xg.at[g_pa, zk], g_pa))):
            send(s, xg.at[g, zk], xsem.at[k * 3], up)
            send(s, xg.at[g, zk], xsem.at[k * 3 + 1], down)

    def both(yy, k):
        return xg.at[pl.ds(yy * 2, 2), zof(k)]

    def xforward(k):
        zk = zof(k)
        arrived(both(ym, k), xsem.at[k * 3])
        arrived(both(yp, k), xsem.at[k * 3 + 1])
        send(xg.at[ym * 2 + c, zk], xg.at[ym * 2 + c, zk], xsem.at[k * 3 + 2], up)
        send(xg.at[yp * 2 + 1 - c, zk], xg.at[yp * 2 + 1 - c, zk], xsem.at[k * 3 + 2], down)

    def hmultiply():
        left_ = jnp.concatenate([xo_h[c].reshape(NZ * 2 * HR, TOK), xh_p[...].reshape(NZ * 2 * HR, TOK)], axis=1)
        for n in range(8):
            r = jnp.concatenate([dyh_o[:, n * FC:(n + 1) * FC], dyh_p[:, n * FC:(n + 1) * FC]], axis=0)
            hp[n] = jnp.dot(left_, r, preferred_element_type=jnp.float32).reshape(NZ, 2, HR, FC)

    def over_z(rows_of, n, s_, r_, sem, last):
        def step(k):
            off = OFFS[k]
            for u in range(2):
                terms = [rows_of(k, u)]
                for i in range(2):
                    if (k, i, u) in HOPS:
                        m = HOPS[k, i, u]
                        arrived(r_.at[m], sem.at[m])
                        terms.append(decoder(r_.at[m], n) if n > 1 else lambda e, m=m: r_[m])
                get = plus(*terms)
                if off == 0:
                    for e in range(n):
                        last(u, e, get(e))
                    continue
                i = u if off == 4 else (0 if off > 0 else 1)
                m = HOPS[OFFS.index((3, -3)[i] if off == 4 else (off - 1 if off > 0 else off + 1)), i, u]
                if n > 1:
                    encode(s_.at[k, u], scales, n, get)
                else:
                    s_[k, u] = get(0)
                send(s_.at[k, u], r_.at[m], sem.at[m], (ahead, behind)[i])
        return step

    def over_x(acc, a_r, s_, b_r, sem):
        way = ((0, xp, right), (1, xm, left))

        def begin():
            for i, x_, dev in way:
                send(acc.at[x2, i], a_r.at[i], sem.at[i], dev)
                send(acc.at[x_, 1 - i], b_r.at[i, 1 - i], sem.at[2], dev)

        def middle():
            for i, x_, dev in way:
                arrived(a_r.at[i], sem.at[i])
                s_[i] = acc[x_, i] + a_r[i]
                send(s_.at[i], b_r.at[i, i], sem.at[2], dev)

        def end(put):
            arrived(b_r, sem.at[2])
            for e in range(2):
                put(e, acc[X, e] + b_r[0, e] + b_r[1, e])
        return begin, middle, end

    def hrows(k, u):
        zk = zof(k)
        return lambda i: hp[(i // 2) * NY + 2 + i % 2, zk, u]

    def hput(u, i, v):
        hr[u * 2 + i // 2, i % 2] = v

    def hyput(e, v):
        hy[2 + e] = v

    hz = over_z(hrows, 4, hz_s, hz_r, hsem, hput)
    hx_begin, hx_middle, hx_end = over_x(hr, ha_r, hs_s, hb_r, hxsem)

    def grows(x_, t):
        return lambda i: hp[(x_ % 2) * NY + i % 2, 2 * t + i // 2, x_ // 2]

    def gsend(src, rcv, sem, dev, get):
        encode(src, scales, 4, get)
        send(src, rcv, sem, dev)

    def gx_begin():
        for t, dev in ((0, right), (2, left), (1, right), (3, left)):
            gsend(ga_s.at[t], ga_r.at[t], gsem.at[t], dev, grows(x2, t))
        for i, t, x_, dev in ((0, 2, xp, right), (1, 0, xm, left), (0, 3, xp, right), (1, 1, xm, left)):
            gsend(gb_s.at[i, t], gb_r.at[i, t], gsem.at[4 + t], dev, grows(x_, t))

    def gx_middle():
        for i, t, x_, dev in ((0, 0, xp, right), (1, 2, xm, left), (0, 1, xp, right), (1, 3, xm, left)):
            arrived(ga_r.at[t], gsem.at[t])
            gsend(gb_s.at[i, t], gb_r.at[i, t], gsem.at[4 + t], dev, plus(grows(x_, t), decoder(ga_r.at[t], 4)))

    def gx_end():
        for t in range(4):
            arrived(gb_r.at[:, t], gsem.at[4 + t])
            get = plus(grows(X, t), decoder(gb_r.at[0, t], 4), decoder(gb_r.at[1, t], 4))
            for i in range(4):
                hq[i % 2, 2 * t + i // 2] = get(i)

    def qrows(k, u):
        zk = zof(k)
        return lambda e: hq[u, zk]

    def qput(u, e, v):
        hy[u] = v

    gz = over_z(qrows, 1, hq_s, hq_r, qsem, qput)

    def hy_begin():
        send(hy.at[y2], hy_r.at[0], tsem.at[3], up)
        send(hy.at[ym], hy_r.at[2], tsem.at[4], down)

    def hy_middle():
        arrived(hy_r.at[0], tsem.at[3])
        hy_s[...] = hy[yp] + hy_r[0]
        send(hy_s, hy_r.at[1], tsem.at[5], up)

    def hy_end():
        arrived(hy_r.at[2], tsem.at[4])
        arrived(hy_r.at[1], tsem.at[5])
        res[0] = hy[y] + hy_r[1] + hy_r[2]

    def multiply(k):
        b, zk = k, zof(k)
        for q in range(NG // GG):
            for h in range(2):
                v = jnp.concatenate([xg[q * GG + i, zk, h] for i in range(GG)], axis=1)
                for e in range(NC):
                    lhs[(h * NC + e) * HR:(h * NC + e + 1) * HR, :] = v * msk[q, e:e + 1, :].astype(v.dtype)
            for j in range(2):
                r = jnp.dot(lhs[...], dyg[j, q * GG * TOK:(q + 1) * GG * TOK, :], preferred_element_type=jnp.float32)
                r = r.reshape(2, NC * HR, FC)
                part[b, j] = r if q == 0 else part[b, j] + r

    def rows(k, x_, h):
        return lambda e: part[k, x_ % 2, x_ // 2, (h * NB[0] + e) * HR:(h * NB[0] + e + 1) * HR, :]

    def compute(k):
        multiply(k)
        for h, dev in ((0, right), (1, left)):
            encode(xa_s.at[k, h], scales, NB[h], rows(k, x2, h))
            send(xa_s.at[k, h, span(NB[h])], xa_r.at[k, h, span(NB[h])], asem.at[k * 2 + h], dev)
        for i, h, x_, dev in ((0, 1, xp, right), (1, 0, xm, left)):
            encode(xb_s.at[k, i, h], scales, NB[h], rows(k, x_, h))
            send(xb_s.at[k, i, h, span(NB[h])], xb_r.at[k, i, h, span(NB[h])], bsem.at[k * 2 + h], dev)

    def xsum(k):
        for h, x_, dev in ((0, xp, right), (1, xm, left)):
            arrived(xa_r.at[k, h, span(NB[h])], asem.at[k * 2 + h])
            encode(xb_s.at[k, h, h], scales, NB[h], plus(rows(k, x_, h), decoder(xa_r.at[k, h], NB[h])))
            send(xb_s.at[k, h, h, span(NB[h])], xb_r.at[k, h, h, span(NB[h])], bsem.at[k * 2 + h], dev)

    def zsum(k):
        off = OFFS[k]
        for h in range(2):
            n = NB[h]
            arrived(xb_r.at[k, :, h, span(n)], bsem.at[k * 2 + h])
            terms = [rows(k, X, h), decoder(xb_r.at[k, 0, h], n), decoder(xb_r.at[k, 1, h], n)]
            for i in range(2):
                if (k, i, h) in HOPS:
                    m = HOPS[k, i, h]
                    arrived(z_r.at[m, span(n)], zsem.at[m])
                    terms.append(decoder(z_r.at[m], n))
            get = plus(*terms)
            if off == 0:
                for e in range(n):
                    res[1 + h * NB[0] + e] = get(e)
                continue
            encode(z_s.at[k, h], scales, n, get)
            i = h if off == 4 else (0 if off > 0 else 1)
            m = HOPS[OFFS.index((3, -3)[i] if off == 4 else (off - 1 if off > 0 else off + 1)), i, h]
            send(z_s.at[k, h, span(n)], z_r.at[m, span(n)], zsem.at[m], (ahead, behind)[i])

    def czrows(k, u):
        return lambda i: part[k, i // 2, u, (NX1 + i % 2) * HR:(NX1 + i % 2 + 1) * HR, :]

    def czput(u, i, v):
        cr[u * 2 + i // 2, i % 2] = v

    def cxput(e, v):
        res[1 + NX1 + e] = v

    czsum = over_z(czrows, 4, cz_s, cz_r, csem, czput)
    cx_begin, cx_middle, cx_end = over_x(cr, cxa_r, cx_s, cxb_r, cxsem)

    arrived(xh_p, tsem.at[1])
    arrived(dyh_p, tsem.at[0])
    hmultiply()
    gx_begin()
    hz(0)
    for g in range(NG):
        for j, (_, owner) in enumerate(cold_blocks(g)):
            for e in range(NC):
                name = e + jnp.where(e >= hot, 1, 0)
                lanes = slice((g % GG) * TOK + j * BLOCK, (g % GG) * TOK + (j + 1) * BLOCK)
                msk[g // GG, e:e + 1, lanes] = jnp.full((1, BLOCK), flag(owner == name), jnp.float32)
    arrived(xg.at[g_pa], tsem.at[2])
    xsend(0)
    arrived(rel.at[0], dsem.at[0])
    send(rel.at[0], dyslot(0, ym * 2 + c), dsem.at[7], up)
    arrived(rel.at[1], dsem.at[1])
    send(rel.at[1], dyslot(1, yp * 2 + c), dsem.at[8], down)
    hz(1)
    hz(2)
    gd, gu, gf = ym * 2 + c, yp * 2 + c, y2 * 2 + c

    def relay(g, j, i):
        arrived(dyslot(j, g), dsem.at[i])
        send(dyslot(j, g), dyslot(j, g), dsem.at[6], partner)

    relay(gd, 0, 2)
    relay(gu, 0, 4)
    gx_middle()
    relay(gd, 1, 3)
    relay(gu, 1, 5)
    xforward(0)
    xsend(1)
    xsend(2)
    relay(gf, 0, 7)
    relay(gf, 1, 8)
    hz(3)
    hz(4)
    arrived(dyg.at[0], dsem.at[6])

    def chunk(k):
        arrived(both(y2, k), xsem.at[k * 3 + 2])
        compute(k)
        if k < NZ - 2:
            xforward(k + 2)
        if k < NZ - 4:
            xsend(k + 4)

    xforward(1)
    xsend(3)
    chunk(0)
    czsum(0)
    gx_end()
    gz(0)
    chunk(1)
    gz(1)
    gz(2)
    hz(5)
    hz(6)
    chunk(2)
    xsum(0)
    czsum(1)
    czsum(2)
    chunk(3)
    xsum(1)
    gz(3)
    gz(4)
    hz(7)
    hx_begin()
    chunk(4)
    xsum(2)
    zsum(0)
    czsum(3)
    czsum(4)
    chunk(5)
    xsum(3)
    gz(5)
    gz(6)
    hx_middle()
    chunk(6)
    xsum(4)
    zsum(1)
    zsum(2)
    czsum(5)
    czsum(6)
    chunk(7)
    xsum(5)
    gz(7)
    hx_end(hyput)
    hy_begin()
    xsum(6)
    zsum(3)
    zsum(4)
    czsum(7)
    cx_begin()
    xsum(7)
    hy_middle()
    zsum(5)
    cx_middle()
    zsum(6)
    hy_end()
    cx_end(cxput)
    zsum(7)
    for e in range(NE):
        v = res[0] * flag(e == hot)
        if e < NC:
            v = v + res[1 + e] * flag(e < hot)
        if e > 0:
            v = v + res[e] * flag(e > hot)
        out[e] = v
    for op in started:
        op.wait_send()


def shards(x_rows, dy_rows, seg_blocks):
    bf16, f32, i16 = jnp.bfloat16, jnp.float32, jnp.int16
    vm = pl.BlockSpec(memory_space=pltpu.VMEM)
    sem = pltpu.SemaphoreType.DMA
    nh = len(HOPS)
    return pl.pallas_call(
        kernel,
        out_shape=pltpu.VMEM((NE, HR, FC), f32),
        in_specs=[pl.BlockSpec(memory_space=pl.ANY)] * 3,
        out_specs=vm,
        scratch_shapes=[
            pltpu.SMEM((NE, seg_blocks.shape[0]), jnp.int32),
            pltpu.VMEM((NE, seg_blocks.shape[0]), jnp.int32),
            pltpu.VMEM(x_rows.shape, bf16),
            pltpu.VMEM(dy_rows.shape, bf16),
            pltpu.VMEM((NG // GG, NE, GG * TOK), f32),
            pltpu.VMEM((2, NZ, 2, HR, TOK), bf16),
            pltpu.VMEM((2, NZ, 2, HR, TOK), bf16),
            pltpu.VMEM((NZ, 2, HR, TOK), bf16),
            pltpu.VMEM((NG, NZ, 2, HR, TOK), bf16),
            pltpu.VMEM((TOK, 8 * FC), bf16),
            pltpu.VMEM((TOK, 8 * FC), bf16),
            pltpu.VMEM((TOK, 8 * FC), bf16),
            pltpu.VMEM((2, NG * TOK, FC), bf16),
            pltpu.VMEM((2, TOK, FC), bf16),
            pltpu.VMEM((2 * NC * HR, GG * TOK), bf16),
            pltpu.VMEM((NZ, 2, 2, NC * HR, FC), f32),
            pltpu.VMEM((8, NZ, 2, HR, FC), f32),
            pltpu.VMEM((NZ, 2, MSG, FC), i16),
            pltpu.VMEM((NZ, 2, MSG, FC), i16),
            pltpu.VMEM((NZ, 2, 2, MSG, FC), i16),
            pltpu.VMEM((NZ, 2, 2, MSG, FC), i16),
            pltpu.VMEM((NZ, 2, MSG, FC), i16),
            pltpu.VMEM((nh, MSG, FC), i16),
            pltpu.VMEM((NZ, 2, MSG, FC), i16),
            pltpu.VMEM((nh, MSG, FC), i16),
            pltpu.VMEM((4, 2, HR, FC), f32),
            pltpu.VMEM((2, HR, FC), f32),
            pltpu.VMEM((2, HR, FC), f32),
            pltpu.VMEM((2, 2, HR, FC), f32),
            pltpu.VMEM((NZ, 2, MSG, FC), i16),
            pltpu.VMEM((nh, MSG, FC), i16),
            pltpu.VMEM((4, 2, HR, FC), f32),
            pltpu.VMEM((2, HR, FC), f32),
            pltpu.VMEM((2, HR, FC), f32),
            pltpu.VMEM((2, 2, HR, FC), f32),
            pltpu.VMEM((4, MSG, FC), i16),
            pltpu.VMEM((4, MSG, FC), i16),
            pltpu.VMEM((2, 4, MSG, FC), i16),
            pltpu.VMEM((2, 4, MSG, FC), i16),
            pltpu.VMEM((2, NZ, HR, FC), f32),
            pltpu.VMEM((NZ, 2, HR, FC), f32),
            pltpu.VMEM((nh, HR, FC), f32),
            pltpu.VMEM((4, HR, FC), f32),
            pltpu.VMEM((HR, FC), f32),
            pltpu.VMEM((3, HR, FC), f32),
            pltpu.VMEM((16, FC), f32),
            pltpu.VMEM((NE, HR, FC), f32),
            sem((9,)), sem((24,)), sem((16,)), sem((16,)), sem((nh,)), sem((nh,)), sem((3,)),
            sem((nh,)), sem((3,)), sem((8,)), sem((nh,)), sem((6,)), sem((4,)), sem((1,)),
        ],
        compiler_params=pltpu.CompilerParams(
            collective_id=0, has_side_effects=True, vmem_limit_bytes=58 << 20),
    )(seg_blocks.T, x_rows, dy_rows)


def solution(mesh):
    in_specs = (P(("dp", "expert"), None), P(("dp", "expert"), None), P())
    out_specs = P(None, "dp", "expert")
    return jax.shard_map(shards, mesh=mesh, in_specs=in_specs, out_specs=out_specs, check_vma=False)
```

```python
import functools

import jax
import jax.numpy as jnp
from jax import lax
from jax.experimental import pallas as pl
from jax.experimental.pallas import tpu as pltpu
from jax.sharding import PartitionSpec as P

BLOCK = 128
NE = 8
NC = NE - 1
NX1 = 5
NZ1 = NC - NX1
NB = (3, 2)
TOK = 2 * BLOCK
NY, NX, NZ = 4, 4, 8
NG = 2 * NY
GG = 4
HR, FC = 32, 256
MSG = 4 * HR + 16
OFFS = (4, 3, -3, 2, -2, 1, -1, 0)
QMAX = 32700.0


def encode(dst, scales, n, get):
    for e in range(n):
        v = get(e)
        top = jnp.max(jnp.abs(v), axis=0, keepdims=True)
        lev = jnp.ceil(jnp.log2(jnp.maximum(top, 1e-30)) * 256.0) + 1.0
        q = jnp.round(v * (jnp.exp2(lev * (-1.0 / 256.0)) * QMAX))
        dst[e * HR:(e + 1) * HR, :] = q.astype(jnp.int32).astype(jnp.int16)
        scales[e:e + 1, :] = lev
    dst[n * HR:n * HR + 16, :] = scales[...].astype(jnp.int32).astype(jnp.int16)


def decoder(src, n):
    lev = src[n * HR:n * HR + 16, :].astype(jnp.int32).astype(jnp.float32)
    s = jnp.exp2(lev * (1.0 / 256.0)) * (1.0 / QMAX)

    def get(e):
        q = src[e * HR:(e + 1) * HR, :].astype(jnp.int32).astype(jnp.float32)
        return q * s[e:e + 1, :]
    return get


def plus(*gets):
    return lambda e: functools.reduce(lambda p, q: p + q, [g(e) for g in gets])


def span(n):
    return pl.ds(0, n * HR + 16)


def flag(cond):
    return jnp.where(cond, 1.0, 0.0).astype(jnp.float32)


def hops():
    found = {}
    for k, off in enumerate(OFFS):
        for i in range(2):
            if (off if i == 0 else -off) in (0, 1, 2, 3):
                found[k, i] = len(found)
    return found


HOPS = hops()


def kernel(seg_any, x_any, dy_any, out, seg, segv, x, dy, msk, xo_h, xo_c, xh_p, xg, dyh_o, dyh_p, dyc, dyg, rel, lhs, part, hp,
           xa_s, xa_r, xb_s, xb_r, z_s, z_r, cz_s, cz_r, cr, cxa_r, cx_s, cxb_r, hz_s, hz_r, hr, ha_r, hs_s, hb_r,
           ga_s, ga_r, gb_s, gb_r, hq, hq_s, hq_r, hy, hy_s, hy_r, scales, res,
           dsem, xsem, asem, bsem, zsem, csem, cxsem, hsem, hxsem, gsem, qsem, tsem, lsem, ssem):
    dp, ex = lax.axis_index("dp"), lax.axis_index("expert")
    z, xh, c = dp // 4, (dp // 2) % 2, dp % 2
    xl, y = ex // NY, ex % NY
    X = xh * 2 + xl

    def at(z_=z, x_=X, c_=c, y_=y):
        return (z_ * 4 + (x_ // 2) * 2 + c_, (x_ % 2) * NY + y_)

    yp, ym, y2 = (y + 1) % NY, (y + 3) % NY, (y + 2) % NY
    xp, xm, x2 = (X + 1) % NX, (X + 3) % NX, (X + 2) % NX
    zp, zm = (z + 1) % NZ, (z + 7) % NZ
    partner = at(c_=1 - c)
    up, down = at(y_=yp), at(y_=ym)
    right, left = at(x_=xp), at(x_=xm)
    ahead, behind = at(z_=zp), at(z_=zm)
    g_me, g_pa = y * 2 + c, y * 2 + 1 - c

    barrier = pltpu.get_barrier_semaphore()
    for other in (partner, up, down, right, left, ahead, behind):
        pl.semaphore_signal(barrier, inc=1, device_id=other, device_id_type=pl.DeviceIdType.MESH)
    load_dy = pltpu.make_async_copy(dy_any, dy, lsem.at[0])
    load_x = pltpu.make_async_copy(x_any, x, lsem.at[1])
    loads = [pltpu.make_async_copy(seg_any, ref, lsem.at[2 + i]) for i, ref in enumerate((seg, segv))]
    for op in loads:
        op.start()
    load_dy.start()
    load_x.start()
    scales[...] = jnp.zeros_like(scales)

    for op in loads:
        op.wait()

    twos = jnp.min(jnp.where(segv[...] == 2, 1.0, 0.0), axis=1, keepdims=True)
    index = lax.broadcasted_iota(jnp.int32, (NE, 1), 0)
    hot = jnp.min(jnp.where(twos > 0.5, index, NE))

    def cold_blocks(g):
        device = ((dp // 2) * 2 + g % 2) * NG + xl * NY + g // 2
        ends, first, total = [], 0, 0
        for e in range(NE):
            n = seg[e, device]
            total = total + n
            ends.append(total)
            first = first + jnp.where(e < hot, n, 0)
        picked = []
        for j in range(2):
            low = j < first
            at_ = jnp.where(low, j, j + 2)
            owner = 0
            for e in range(NE):
                owner = owner + jnp.where(ends[e] <= at_, 1, 0)
            picked.append((low, owner))
        return picked

    low = [flag(c_[0]) for c_ in cold_blocks(g_me)]

    def pick(ref, j, i, n, width):
        w = low[j] if i == 1 else 1.0 - low[j]
        a, b = ref[j * BLOCK:(j + 1) * BLOCK, n], ref[(j + 2) * BLOCK:(j + 3) * BLOCK, n]
        return (a * jnp.full((1, width), w, jnp.float32).astype(a.dtype)
                + b * jnp.full((1, width), 1.0 - w, jnp.float32).astype(b.dtype))

    def choose(i, dst):
        for j in range(2):
            dst[j * BLOCK:(j + 1) * BLOCK, :] = pick(dy, j, i, slice(0, 8 * FC), 8 * FC)

    load_dy.wait()
    choose(1, dyc)
    pl.semaphore_wait(barrier, 7)

    started = []

    def copy(src, dst, sem, dev):
        return pltpu.make_async_remote_copy(
            src_ref=src, dst_ref=dst, send_sem=ssem.at[0], recv_sem=sem,
            device_id=dev, device_id_type=pl.DeviceIdType.MESH)

    def send(src, dst, sem, dev):
        op = copy(src, dst, sem, dev)
        op.start()
        started.append(op)

    def arrived(dst, sem):
        copy(dst, dst, sem, partner).wait_recv()

    def cols(yy, j):
        return pl.ds(pl.multiple_of((j * NY + yy) * FC, FC), FC)

    def dyslot(j, g):
        return dyg.at[j, pl.ds(pl.multiple_of(g * TOK, TOK), TOK)]

    send(dyc.at[:, cols(y2, 0)], rel.at[0], dsem.at[0], up)
    send(dyc.at[:, cols(y2, 1)], rel.at[1], dsem.at[1], down)
    for j in range(2):
        send(dyc.at[:, cols(yp, j)], dyslot(j, g_me), dsem.at[2 + j], up)
        send(dyc.at[:, cols(ym, j)], dyslot(j, g_me), dsem.at[4 + j], down)
        send(dyc.at[:, cols(y, j)], dyslot(j, g_me), dsem.at[6], partner)
    choose(0, dyh_o)
    send(dyh_o, dyh_p, tsem.at[0], partner)
    for j in range(2):
        dyg[j, pl.ds(pl.multiple_of(g_me * TOK, TOK), TOK)] = dyc[:, cols(y, j)]
    load_x.wait()

    def turn(n, _):
        for j in range(4):
            t = pick(x, j % 2, j // 2, pl.ds(pl.multiple_of(n * BLOCK, BLOCK), BLOCK), BLOCK).T
            dst = (xo_h, xo_c)[j // 2]
            for i in range(4):
                dst[i % 2, n, i // 2, :, (j % 2) * BLOCK:(j % 2 + 1) * BLOCK] = t[i * HR:(i + 1) * HR, :]
        return 0
    lax.fori_loop(0, NZ, turn, 0)
    send(xo_h.at[1 - c], xh_p, tsem.at[1], partner)
    send(xo_c.at[1 - c], xg.at[g_me], tsem.at[2], partner)
    xg[g_me] = xo_c[c]

    def zof(k):
        return (z + OFFS[k] + NZ) % NZ

    def xsend(k):
        zk = zof(k)
        for i, (s, g) in enumerate(((xo_c.at[c, zk], g_me), (xg.at[g_pa, zk], g_pa))):
            send(s, xg.at[g, zk], xsem.at[k * 3], up)
            send(s, xg.at[g, zk], xsem.at[k * 3 + 1], down)

    def both(yy, k):
        return xg.at[pl.ds(yy * 2, 2), zof(k)]

    def xforward(k):
        zk = zof(k)
        arrived(both(ym, k), xsem.at[k * 3])
        arrived(both(yp, k), xsem.at[k * 3 + 1])
        send(xg.at[ym * 2 + c, zk], xg.at[ym * 2 + c, zk], xsem.at[k * 3 + 2], up)
        send(xg.at[yp * 2 + 1 - c, zk], xg.at[yp * 2 + 1 - c, zk], xsem.at[k * 3 + 2], down)

    def hmultiply():
        left_ = jnp.concatenate([xo_h[c].reshape(NZ * 2 * HR, TOK), xh_p[...].reshape(NZ * 2 * HR, TOK)], axis=1)
        for n in range(8):
            r = jnp.concatenate([dyh_o[:, n * FC:(n + 1) * FC], dyh_p[:, n * FC:(n + 1) * FC]], axis=0)
            hp[n] = jnp.dot(left_, r, preferred_element_type=jnp.float32).reshape(NZ, 2, HR, FC)

    def over_z(rows_of, ns, s_, r_, sem, last):
        total = ns[0] + ns[1]

        def step(k):
            off = OFFS[k]
            terms = [[rows_of(k, u)] for u in range(2)]
            for i in range(2):
                if (k, i) in HOPS:
                    m = HOPS[k, i]
                    if off in (3, -3):
                        arrived(r_.at[m, span(ns[i])], sem.at[m])
                        terms[i].append(decoder(r_.at[m], ns[i]))
                    else:
                        arrived(r_.at[m, span(total)], sem.at[m])
                        d = decoder(r_.at[m], total)
                        terms[0].append(d)
                        terms[1].append(lambda e, d=d: d(ns[0] + e))
            halves = [plus(*t) for t in terms]
            if off == 0:
                for u in range(2):
                    for e in range(ns[u]):
                        last(u, e, halves[u](e))
            elif off == 4:
                for u in range(2):
                    m = HOPS[1 + u, u]
                    src = s_.at[(k, NZ)[u]]
                    encode(src, scales, ns[u], halves[u])
                    send(src.at[span(ns[u])], r_.at[m, span(ns[u])], sem.at[m], (ahead, behind)[u])
            else:
                i = 0 if off > 0 else 1
                m = HOPS[OFFS.index(off - 1 if off > 0 else off + 1), i]
                encode(s_.at[k], scales, total, lambda e: halves[0](e) if e < ns[0] else halves[1](e - ns[0]))
                send(s_.at[k, span(total)], r_.at[m, span(total)], sem.at[m], (ahead, behind)[i])
        return step

    def over_x(acc, a_r, s_, b_r, sem):
        n = acc.shape[1]
        cut = (n + 1) // 2
        way = ((pl.ds(0, cut), pl.ds(cut, n - cut), xp, right), (pl.ds(cut, n - cut), pl.ds(0, cut), xm, left))

        def begin():
            for i, (mine, rest, x_, dev) in enumerate(way):
                send(acc.at[x2, mine], a_r.at[mine], sem.at[i], dev)
                send(acc.at[x_, rest], b_r.at[i, rest], sem.at[2], dev)

        def middle():
            for i, (mine, _, x_, dev) in enumerate(way):
                arrived(a_r.at[mine], sem.at[i])
                s_[mine] = acc[x_, mine] + a_r[mine]
                send(s_.at[mine], b_r.at[i, mine], sem.at[2], dev)

        def end(put):
            arrived(b_r, sem.at[2])
            for e in range(n):
                put(e, acc[X, e] + b_r[0, e] + b_r[1, e])
        return begin, middle, end

    def hrows(k, u):
        zk = zof(k)
        return lambda i: hp[(i // 2) * NY + 2 + i % 2, zk, u]

    def hput(u, i, v):
        hr[u * 2 + i // 2, i % 2] = v

    def hyput(e, v):
        hy[2 + e] = v

    hz = over_z(hrows, (4, 4), hz_s, hz_r, hsem, hput)
    hx_begin, hx_middle, hx_end = over_x(hr, ha_r, hs_s, hb_r, hxsem)

    def grows(x_, t):
        return lambda i: hp[(x_ % 2) * NY + i % 2, 2 * t + i // 2, x_ // 2]

    def gsend(src, rcv, sem, dev, get):
        encode(src, scales, 4, get)
        send(src, rcv, sem, dev)

    def gx_begin():
        for t, dev in ((0, right), (2, left), (1, right), (3, left)):
            gsend(ga_s.at[t], ga_r.at[t], gsem.at[t], dev, grows(x2, t))
        for i, t, x_, dev in ((0, 2, xp, right), (1, 0, xm, left), (0, 3, xp, right), (1, 1, xm, left)):
            gsend(gb_s.at[i, t], gb_r.at[i, t], gsem.at[4 + t], dev, grows(x_, t))

    def gx_middle():
        for i, t, x_, dev in ((0, 0, xp, right), (1, 2, xm, left), (0, 1, xp, right), (1, 3, xm, left)):
            arrived(ga_r.at[t], gsem.at[t])
            gsend(gb_s.at[i, t], gb_r.at[i, t], gsem.at[4 + t], dev, plus(grows(x_, t), decoder(ga_r.at[t], 4)))

    def gx_end():
        for t in range(4):
            arrived(gb_r.at[:, t], gsem.at[4 + t])
            get = plus(grows(X, t), decoder(gb_r.at[0, t], 4), decoder(gb_r.at[1, t], 4))
            for i in range(4):
                hq[i % 2, 2 * t + i // 2] = get(i)

    def qrows(k, u):
        zk = zof(k)
        return lambda e: hq[u, zk]

    def qput(u, e, v):
        hy[u] = v

    gz = over_z(qrows, (1, 1), hq_s, hq_r, qsem, qput)

    def hy_begin():
        send(hy.at[y2], hy_r.at[0], tsem.at[3], up)
        send(hy.at[ym], hy_r.at[2], tsem.at[4], down)

    def hy_middle():
        arrived(hy_r.at[0], tsem.at[3])
        hy_s[...] = hy[yp] + hy_r[0]
        send(hy_s, hy_r.at[1], tsem.at[5], up)

    def hy_end():
        arrived(hy_r.at[2], tsem.at[4])
        arrived(hy_r.at[1], tsem.at[5])
        res[0] = hy[y] + hy_r[1] + hy_r[2]

    def multiply(k):
        b, zk = k, zof(k)
        for q in range(NG // GG):
            for h in range(2):
                v = jnp.concatenate([xg[q * GG + i, zk, h] for i in range(GG)], axis=1)
                for e in range(NC):
                    lhs[(h * NC + e) * HR:(h * NC + e + 1) * HR, :] = v * msk[q, e:e + 1, :].astype(v.dtype)
            for j in range(2):
                r = jnp.dot(lhs[...], dyg[j, q * GG * TOK:(q + 1) * GG * TOK, :], preferred_element_type=jnp.float32)
                r = r.reshape(2, NC * HR, FC)
                part[b, j] = r if q == 0 else part[b, j] + r

    def rows(k, x_, h):
        return lambda e: part[k, x_ % 2, x_ // 2, (h * NB[0] + e) * HR:(h * NB[0] + e + 1) * HR, :]

    def compute(k):
        multiply(k)
        for i, x_, dev in ((0, xp, right), (1, xm, left)):
            far, near = rows(k, x2, i), rows(k, x_, 1 - i)
            encode(xa_s.at[k, i], scales, NX1, lambda e: far(e) if e < NB[i] else near(e - NB[i]))
            send(xa_s.at[k, i, span(NX1)], xa_r.at[k, i, span(NX1)], asem.at[k * 2 + i], dev)

    def xsum(k):
        for h, x_, dev in ((0, xp, right), (1, xm, left)):
            arrived(xa_r.at[k, h, span(NX1)], asem.at[k * 2 + h])
            encode(xb_s.at[k, h], scales, NB[h], plus(rows(k, x_, h), decoder(xa_r.at[k, h], NX1)))
            send(xb_s.at[k, h, span(NB[h])], xb_r.at[k, h, span(NB[h])], bsem.at[k * 2 + h], dev)

    def xrows(k, h):
        arrived(xb_r.at[k, h, span(NB[h])], bsem.at[k * 2 + h])
        d = decoder(xa_r.at[k, 1 - h], NX1)
        return plus(rows(k, X, h), decoder(xb_r.at[k, h], NB[h]), lambda e: d(NB[1 - h] + e))

    def xput(h, e, v):
        res[1 + h * NB[0] + e] = v

    zsum = over_z(xrows, NB, z_s, z_r, zsem, xput)

    def czrows(k, u):
        return lambda i: part[k, i // NZ1, u, (NX1 + i % NZ1) * HR:(NX1 + i % NZ1 + 1) * HR, :]

    def czput(u, i, v):
        cr[u * 2 + i // NZ1, i % NZ1] = v

    def cxput(e, v):
        res[1 + NX1 + e] = v

    czsum = over_z(czrows, (2 * NZ1, 2 * NZ1), cz_s, cz_r, csem, czput)
    cx_begin, cx_middle, cx_end = over_x(cr, cxa_r, cx_s, cxb_r, cxsem)

    arrived(xh_p, tsem.at[1])
    arrived(dyh_p, tsem.at[0])
    hmultiply()
    gx_begin()
    hz(0)
    for g in range(NG):
        for j, (_, owner) in enumerate(cold_blocks(g)):
            for e in range(NC):
                name = e + jnp.where(e >= hot, 1, 0)
                lanes = slice((g % GG) * TOK + j * BLOCK, (g % GG) * TOK + (j + 1) * BLOCK)
                msk[g // GG, e:e + 1, lanes] = jnp.full((1, BLOCK), flag(owner == name), jnp.float32)
    arrived(xg.at[g_pa], tsem.at[2])
    xsend(0)
    arrived(rel.at[0], dsem.at[0])
    send(rel.at[0], dyslot(0, ym * 2 + c), dsem.at[7], up)
    arrived(rel.at[1], dsem.at[1])
    send(rel.at[1], dyslot(1, yp * 2 + c), dsem.at[8], down)
    hz(1)
    hz(2)
    gd, gu, gf = ym * 2 + c, yp * 2 + c, y2 * 2 + c

    def relay(g, j, i):
        arrived(dyslot(j, g), dsem.at[i])
        send(dyslot(j, g), dyslot(j, g), dsem.at[6], partner)

    relay(gd, 0, 2)
    relay(gu, 0, 4)
    gx_middle()
    relay(gd, 1, 3)
    relay(gu, 1, 5)
    xforward(0)
    xsend(1)
    xsend(2)
    relay(gf, 0, 7)
    relay(gf, 1, 8)
    hz(3)
    hz(4)
    arrived(dyg.at[0], dsem.at[6])

    def chunk(k):
        arrived(both(y2, k), xsem.at[k * 3 + 2])
        compute(k)
        if k < NZ - 2:
            xforward(k + 2)
        if k < NZ - 4:
            xsend(k + 4)

    xforward(1)
    xsend(3)
    chunk(0)
    czsum(0)
    gx_end()
    gz(0)
    chunk(1)
    hz(5)
    hz(6)
    chunk(2)
    gz(1)
    gz(2)
    xsum(0)
    czsum(1)
    czsum(2)
    chunk(3)
    xsum(1)
    chunk(4)
    xsum(2)
    hz(7)
    hx_begin()
    gz(3)
    gz(4)
    zsum(0)
    czsum(3)
    czsum(4)
    chunk(5)
    xsum(3)
    gz(5)
    gz(6)
    hx_middle()
    chunk(6)
    xsum(4)
    zsum(1)
    zsum(2)
    czsum(5)
    czsum(6)
    chunk(7)
    xsum(5)
    gz(7)
    xsum(6)
    zsum(3)
    zsum(4)
    czsum(7)
    cx_begin()
    hx_end(hyput)
    hy_begin()
    xsum(7)
    cx_middle()
    zsum(5)
    hy_middle()
    zsum(6)
    cx_end(cxput)
    hy_end()
    zsum(7)
    for e in range(NE):
        v = res[0] * flag(e == hot)
        if e < NC:
            v = v + res[1 + e] * flag(e < hot)
        if e > 0:
            v = v + res[e] * flag(e > hot)
        out[e] = v
    for op in started:
        op.wait_send()


def shards(x_rows, dy_rows, seg_blocks):
    bf16, f32, i16 = jnp.bfloat16, jnp.float32, jnp.int16
    vm = pl.BlockSpec(memory_space=pltpu.VMEM)
    sem = pltpu.SemaphoreType.DMA
    nh = len(HOPS)
    return pl.pallas_call(
        kernel,
        out_shape=pltpu.VMEM((NE, HR, FC), f32),
        in_specs=[pl.BlockSpec(memory_space=pl.ANY)] * 3,
        out_specs=vm,
        scratch_shapes=[
            pltpu.SMEM((NE, seg_blocks.shape[0]), jnp.int32),
            pltpu.VMEM((NE, seg_blocks.shape[0]), jnp.int32),
            pltpu.VMEM(x_rows.shape, bf16),
            pltpu.VMEM(dy_rows.shape, bf16),
            pltpu.VMEM((NG // GG, NE, GG * TOK), f32),
            pltpu.VMEM((2, NZ, 2, HR, TOK), bf16),
            pltpu.VMEM((2, NZ, 2, HR, TOK), bf16),
            pltpu.VMEM((NZ, 2, HR, TOK), bf16),
            pltpu.VMEM((NG, NZ, 2, HR, TOK), bf16),
            pltpu.VMEM((TOK, 8 * FC), bf16),
            pltpu.VMEM((TOK, 8 * FC), bf16),
            pltpu.VMEM((TOK, 8 * FC), bf16),
            pltpu.VMEM((2, NG * TOK, FC), bf16),
            pltpu.VMEM((2, TOK, FC), bf16),
            pltpu.VMEM((2 * NC * HR, GG * TOK), bf16),
            pltpu.VMEM((NZ, 2, 2, NC * HR, FC), f32),
            pltpu.VMEM((8, NZ, 2, HR, FC), f32),
            pltpu.VMEM((NZ, 2, NX1 * HR + 16, FC), i16),
            pltpu.VMEM((NZ, 2, NX1 * HR + 16, FC), i16),
            pltpu.VMEM((NZ, 2, MSG, FC), i16),
            pltpu.VMEM((NZ, 2, MSG, FC), i16),
            pltpu.VMEM((NZ + 1, 5 * HR + 16, FC), i16),
            pltpu.VMEM((nh, 5 * HR + 16, FC), i16),
            pltpu.VMEM((NZ + 1, 4 * NZ1 * HR + 16, FC), i16),
            pltpu.VMEM((nh, 4 * NZ1 * HR + 16, FC), i16),
            pltpu.VMEM((4, NZ1, HR, FC), f32),
            pltpu.VMEM((NZ1, HR, FC), f32),
            pltpu.VMEM((NZ1, HR, FC), f32),
            pltpu.VMEM((2, NZ1, HR, FC), f32),
            pltpu.VMEM((NZ + 1, 8 * HR + 16, FC), i16),
            pltpu.VMEM((nh, 8 * HR + 16, FC), i16),
            pltpu.VMEM((4, 2, HR, FC), f32),
            pltpu.VMEM((2, HR, FC), f32),
            pltpu.VMEM((2, HR, FC), f32),
            pltpu.VMEM((2, 2, HR, FC), f32),
            pltpu.VMEM((4, MSG, FC), i16),
            pltpu.VMEM((4, MSG, FC), i16),
            pltpu.VMEM((2, 4, MSG, FC), i16),
            pltpu.VMEM((2, 4, MSG, FC), i16),
            pltpu.VMEM((2, NZ, HR, FC), f32),
            pltpu.VMEM((NZ + 1, 2 * HR + 16, FC), i16),
            pltpu.VMEM((nh, 2 * HR + 16, FC), i16),
            pltpu.VMEM((4, HR, FC), f32),
            pltpu.VMEM((HR, FC), f32),
            pltpu.VMEM((3, HR, FC), f32),
            pltpu.VMEM((16, FC), f32),
            pltpu.VMEM((NE, HR, FC), f32),
            sem((9,)), sem((24,)), sem((16,)), sem((16,)), sem((nh,)), sem((nh,)), sem((3,)),
            sem((nh,)), sem((3,)), sem((8,)), sem((nh,)), sem((6,)), sem((4,)), sem((1,)),
        ],
        compiler_params=pltpu.CompilerParams(
            collective_id=0, has_side_effects=True, vmem_limit_bytes=58 << 20),
    )(seg_blocks.T, x_rows, dy_rows)


def solution(mesh):
    in_specs = (P(("dp", "expert"), None), P(("dp", "expert"), None), P())
    out_specs = P(None, "dp", "expert")
    return jax.shard_map(shards, mesh=mesh, in_specs=in_specs, out_specs=out_specs, check_vma=False)
```
